32 devices in a mesh: row: 8 (over z, x), col: 4 (over y, core).
Axes of the slice: x: 2, y: 2, z: 4, core: 2. Of those that a mesh axis runs over, the one named last changes fastest.
Arguments:
- source_points: bfloat16 [512, 64, 128], P(('row', 'col')), may hold values from -1.5 to 1.5
- target_points: bfloat16 [512, 64, 128], P(('row', 'col')), may hold values from -1.5 to 1.5
- source_mass: float32 [512, 128], P(('row', 'col')), may hold values from -4 to 4
- target_mass: float32 [512, 128], P(('row', 'col')), may hold values from -4 to 4
- support: int32 [512, 32], P(('row', 'col')), may hold values from 0 to 511, as said below
- coarse_potential: float32 [512, 128], P(('row', 'col')), may hold values from -4 to 150
Outputs:
- potential_f: float32 [512, 128], P(('row', 'col'))
- potential_g: float32 [512, 128], P(('row', 'col'))
The draws below stay inside these ranges and needn't reach their ends.
Inputs may be any that keep to these rules, and one draw needn't show every extreme that they name: `support`: each row names 32 different target clusters. The rows of one device's 16 source clusters name, among the 16 target clusters of any one device, exactly 2 different ones. Every target cluster is named by some row.
All inputs are finite; a program needn't handle non-finite values.
Results may differ from the reference program's by a relative error of at most 0.0003.
Values may be sent and summed in bfloat16 or wider, within the bound.
A program may use at most 64 MiB of HBM per device.

```python
import jax
import jax.numpy as jnp
from jax import lax

D = 64
PTS = 128
SUP = 32
CAP = 2
ITERS = 2
CL_DEV = 16
SRC_CL = 512
TGT_CL = 512
DEVICES = 32


def shuffle(subkey):
    return jax.random.permutation(subkey, DEVICES * CAP)


def pick_some(subkey):
    return jax.random.permutation(subkey, DEVICES * CAP)[:SUP]


def reorder(subkey):
    return jax.random.permutation(subkey, CL_DEV)


def draw_support(key, part):
    listed = DEVICES * CAP
    covering = -(-listed // SUP)
    offsets = jax.random.randint(jax.random.fold_in(key, 11), (DEVICES,), 0, CL_DEV)
    subkeys = jax.random.split(jax.random.fold_in(key, 12), DEVICES)
    orders = jax.vmap(shuffle)(subkeys)
    owners = orders // CAP
    within = orders % CAP
    requester = jnp.arange(DEVICES)[:, None]
    local = (requester * CAP + within + offsets[owners]) % CL_DEV
    entries = owners * CL_DEV + local
    row_ids = jnp.arange(CL_DEV)
    periodic = (row_ids[:, None] * SUP + jnp.arange(SUP)[None, :]) % listed
    row_keys = jax.random.split(jax.random.fold_in(key, 13), DEVICES * CL_DEV)
    scattered = jax.vmap(pick_some)(row_keys).reshape(DEVICES, CL_DEV, SUP)
    position = jnp.where(row_ids[None, :, None] < covering, periodic[None, :, :], scattered)
    row_orders = jax.vmap(reorder)(jax.random.split(jax.random.fold_in(key, 14), DEVICES))
    position = jnp.take_along_axis(position, row_orders[:, :, None], axis=1)
    chosen = jnp.take_along_axis(entries, position.reshape(DEVICES, CL_DEV * SUP), axis=1)
    return chosen.reshape(DEVICES * CL_DEV, SUP).astype(jnp.int32)


def feature_signs(key):
    flips = jax.random.randint(jax.random.fold_in(key, 31), (D,), 0, 2)
    return (2 * flips - 1).astype(jnp.float32)


def draw_embedded(key, salt):
    shape = (CL_DEV * DEVICES, D, PTS)
    offset = 0.6 * feature_signs(key)[None, :, None]
    noise = 0.25 * jax.random.normal(jax.random.fold_in(key, salt), shape, jnp.float32)
    return jnp.clip(noise + offset, -1.5, 1.5).astype(jnp.bfloat16)


def draw_source_points(key, part):
    return draw_embedded(key, 41)


def draw_target_points(key, part):
    return draw_embedded(key, 42)


def draw_coarse_potential(key, part):
    shape = (CL_DEV * DEVICES, PTS)
    return jnp.clip(jax.random.normal(jax.random.fold_in(key, 24), shape, jnp.float32), -4.0, 4.0)


def block_levels(rng, shape, cuts, low, largest):
    gain, own = 1.0, jax.random.fold_in(rng, 6)
    for dim, blocks in cuts:
        heights = jnp.exp(jax.random.uniform(jax.random.fold_in(own, dim), (blocks,), jnp.float32, low / len(cuts), largest / len(cuts)))
        gain = gain * jnp.repeat(heights, shape[dim] // blocks).reshape([-1 if axis == dim else 1 for axis in range(len(shape))])
    return gain


def centred(key, shape, width, limit, pieces=(), held_as=jnp.bfloat16):
    level = block_levels(key, shape, pieces, -0.22, 0.18) if pieces else 1.0
    array = jax.random.normal(key, shape, jnp.float32) * width * level
    return jnp.minimum(jnp.maximum(array, -limit), limit).astype(held_as)


def setup_inputs(seed: int = 0) -> dict:
    keys = jax.random.split(jax.random.key(seed), 7)
    source_points = draw_source_points(jax.random.fold_in(keys[6], 71), 0)
    target_points = draw_target_points(jax.random.fold_in(keys[6], 71), 0)
    source_mass = centred(keys[2], (SRC_CL, PTS), 1.0, 4.0, ((0, 32),), jnp.float32)
    target_mass = centred(keys[3], (TGT_CL, PTS), 1.0, 4.0, ((0, 32),), jnp.float32)
    support = draw_support(jax.random.fold_in(keys[6], 71), 0)
    coarse_potential = draw_coarse_potential(jax.random.fold_in(keys[6], 71), 0)
    return dict(source_points=source_points, target_points=target_points, source_mass=source_mass, target_mass=target_mass, support=support, coarse_potential=coarse_potential)


epsilon = 0.5
lowest = -1e30


def squares(points):
    wide = points.astype(jnp.float32)
    return jnp.sum(wide * wide, axis=-2)


def cluster_terms(source, source_sq, source_log, tiles, tiles_sq, shifted):
    cross = jnp.einsum("dp,tdq->tpq", source.astype(jnp.float32), tiles.astype(jnp.float32))
    cost = source_sq[None, :, None] + tiles_sq[:, None, :] - 2.0 * cross
    scores = (shifted[:, None, :] - cost) / epsilon
    peak = jnp.max(scores, axis=(0, 2))
    total = jnp.sum(jnp.exp(scores - peak[None, :, None]), axis=(0, 2))
    potential = -epsilon * (peak + jnp.log(total))
    lifted = potential + epsilon * source_log
    backward = (lifted[None, :, None] - cost) / epsilon
    column_peak = jnp.max(backward, axis=1)
    column_total = jnp.sum(jnp.exp(backward - column_peak[:, None, :]), axis=1)
    return potential, column_peak, column_total


def fold_max(old_max, old_sum, new_max, new_sum):
    upper = jnp.maximum(old_max, new_max)
    return upper, old_sum * jnp.exp(old_max - upper) + new_sum * jnp.exp(new_max - upper)


def reference(source_points, target_points, source_mass, target_mass, support, coarse_potential):
    source_sq = squares(source_points)
    target_sq = squares(target_points)
    potential_g = coarse_potential
    potential_f = jnp.zeros(source_mass.shape, jnp.float32)
    for sweep in range(ITERS):
        shifted_all = potential_g + epsilon * target_mass

        def visit(carry, item):
            run_max, run_sum = carry
            source, sq_row, log_row, targets = item
            potential, column_peak, column_total = cluster_terms(
                source, sq_row, log_row, target_points[targets], target_sq[targets], shifted_all[targets])
            upper, summed = fold_max(run_max[targets], run_sum[targets], column_peak, column_total)
            return (run_max.at[targets].set(upper), run_sum.at[targets].set(summed)), potential

        start = (jnp.full(coarse_potential.shape, lowest, jnp.float32), jnp.zeros(coarse_potential.shape, jnp.float32))
        (run_max, run_sum), potential_f = lax.scan(visit, start, (source_points, source_sq, source_mass, support))
        potential_g = -epsilon * (run_max + jnp.log(run_sum))
    return potential_f, potential_g
```

```python
import functools

import jax
import jax.numpy as jnp
from jax import lax
from jax.experimental import pallas as pl
from jax.experimental.pallas import tpu as pltpu
from jax.sharding import PartitionSpec as P

CAP = 2
EXTRA = 16
LIFT = 20.0
FLOOR = 1e-10
ALARM = 3e38
ITERS = 2
AXES = ("row", "col")
GROUP = 4
MESH = pl.DeviceIdType.MESH


epsilon = 0.5
lowest = -1e30


def squares(points):
    wide = points.astype(jnp.float32)
    return jnp.sum(wide * wide, axis=-2)


def pieces(row, depth):
    high = row.astype(jnp.bfloat16).astype(jnp.float32)
    rest = row - high
    middle = rest.astype(jnp.bfloat16).astype(jnp.float32)
    low = rest - middle
    index = lax.broadcasted_iota(jnp.int32, (depth, row.shape[1]), 0)
    return jnp.where(
        index == 0, high, jnp.where(index == 1, middle, jnp.where(index == 2, low, 0.0))
    )


def ones_rows(depth, points):
    index = lax.broadcasted_iota(jnp.int32, (depth, points), 0)
    return jnp.where(index < 3, 1.0, 0.0)


def fold(old_max, old_sum, scores):
    rows, lanes = scores.shape
    blocks = scores.reshape(rows // 8, 8, lanes)
    upper = jnp.maximum(old_max, jnp.max(blocks, axis=0))
    total = old_sum * jnp.exp(old_max - upper) + jnp.sum(jnp.exp(blocks - upper[None]), axis=0)
    return upper, total


def sweep_kernel(
    slots_ref, source_ref, mass_ref, tiles_ref, u_ref, row_ref, column_ref,
    tile_forward, tile_backward, run_max, run_sum,
):
    clusters, features, points = source_ref.shape
    slots = tiles_ref.shape[0]
    entries = slots_ref.shape[1]
    spare = tile_forward.shape[2] - features
    ones = ones_rows(spare, points)

    def prepare(slot, carry):
        tile = tiles_ref[slot].astype(jnp.float32)
        extra = pieces(u_ref[pl.ds(slot, 1), :], spare)
        tile_forward[slot] = jnp.concatenate([4.0 * tile, extra], axis=0).T.astype(jnp.bfloat16)
        tile_backward[slot] = jnp.concatenate([tile, ones], axis=0).astype(jnp.bfloat16)
        run_max[slot] = jnp.full((8, points), lowest, jnp.float32)
        run_sum[slot] = jnp.zeros((8, points), jnp.float32)
        return carry

    lax.fori_loop(0, slots, prepare, 0, unroll=8)

    def visit(cluster, carry):
        source = source_ref[cluster].astype(jnp.float32)
        right = jnp.concatenate([source, ones], axis=0).astype(jnp.bfloat16)

        def forward(step, state):
            lhs = jnp.concatenate(
                [tile_forward[slots_ref[cluster, step * GROUP + lane]] for lane in range(GROUP)],
                axis=0,
            )
            return fold(*state, jnp.dot(lhs, right, preferred_element_type=jnp.float32))

        start = (
            jnp.full((8, points), lowest, jnp.float32),
            jnp.zeros((8, points), jnp.float32),
        )
        upper, total = lax.fori_loop(0, entries // GROUP, forward, start, unroll=True)
        peak = jnp.max(upper, axis=0, keepdims=True)
        total = jnp.sum(total * jnp.exp(upper - peak), axis=0, keepdims=True)
        level = peak + jnp.log(total)
        row_ref[pl.ds(cluster, 1), :] = level
        extra = pieces(mass_ref[pl.ds(cluster, 1), :] - level, spare)
        left = jnp.concatenate([4.0 * source, extra], axis=0).T.astype(jnp.bfloat16)

        def backward(step, state):
            chosen = [slots_ref[cluster, step * GROUP + lane] for lane in range(GROUP)]
            held = [(run_max[slot], run_sum[slot]) for slot in chosen]
            rhs = jnp.concatenate([tile_backward[slot] for slot in chosen], axis=1)
            scores = jnp.dot(left, rhs, preferred_element_type=jnp.float32)
            fresh = [
                fold(*held[lane], scores[:, lane * points : (lane + 1) * points])
                for lane in range(GROUP)
            ]
            for slot, (new_max, new_sum) in zip(chosen, fresh):
                run_max[slot] = new_max
                run_sum[slot] = new_sum
            return state

        lax.fori_loop(0, entries // GROUP, backward, 0, unroll=True)
        return carry

    lax.fori_loop(0, clusters, visit, 0)
    upper = run_max[...]
    peak = jnp.max(upper, axis=1, keepdims=True)
    total = jnp.sum(run_sum[...] * jnp.exp(upper - peak), axis=1)
    column_ref[...] = peak[:, 0] + jnp.log(total)


def sweep_call(slot_list, source, mass, tiles, u):
    clusters, features, points = source.shape
    slots = tiles.shape[0]
    depth = 2 * features
    vmem = pl.BlockSpec(memory_space=pltpu.VMEM)
    pairs = clusters * slot_list.shape[1]
    return pl.pallas_call(
        sweep_kernel,
        out_shape=(
            jax.ShapeDtypeStruct((clusters, points), jnp.float32),
            jax.ShapeDtypeStruct((slots, points), jnp.float32),
        ),
        in_specs=[pl.BlockSpec(memory_space=pltpu.SMEM), vmem, vmem, vmem, vmem],
        out_specs=(vmem, vmem),
        scratch_shapes=[
            pltpu.VMEM((slots, points, depth), jnp.bfloat16),
            pltpu.VMEM((slots, depth, points), jnp.bfloat16),
            pltpu.VMEM((slots, 8, points), jnp.float32),
            pltpu.VMEM((slots, 8, points), jnp.float32),
        ],
        cost_estimate=pl.CostEstimate(
            flops=4 * pairs * points * points * depth,
            transcendentals=2 * pairs * points * points,
            bytes_accessed=2 * slots * features * points,
        ),
        name="sweep",
    )(slot_list, source, mass, tiles, u)


def place():
    rows, columns = lax.axis_size("row"), lax.axis_size("col")
    return lax.axis_index("row") * columns + lax.axis_index("col"), rows * columns, columns


def peer_of(step):
    me, devices, columns = place()
    peer = lax.rem(me + step, devices)
    return peer, (lax.div(peer, columns), lax.rem(peer, columns))


def greet():
    devices = place()[1]
    barrier = pltpu.get_barrier_semaphore()

    def signal(step, carry):
        pl.semaphore_signal(barrier, inc=1, device_id=peer_of(step)[1], device_id_type=MESH)
        return carry

    lax.fori_loop(1, devices, signal, 0, unroll=8)
    pl.semaphore_wait(barrier, devices - 1)


def send_all(sources, targets, send_sem, recv_sem, first):
    me, devices, _ = place()

    def send(step, carry):
        peer, where = peer_of(step)
        for index, (source, target) in enumerate(zip(sources, targets)):
            pltpu.make_async_remote_copy(
                src_ref=source.at[peer],
                dst_ref=target.at[me],
                send_sem=send_sem.at[first + index],
                recv_sem=recv_sem.at[first + index],
                device_id=where,
                device_id_type=MESH,
            ).start()
        return carry

    lax.fori_loop(1, devices, send, 0, unroll=8)
    for source, target in zip(sources, targets):
        target[me] = source[me]


def wait_all(refs, sems, first):
    devices = place()[1]
    for index, ref in enumerate(refs):
        blocks = ref.at[pl.ds(0, devices - 1)]
        pltpu.make_async_copy(blocks, blocks, sems.at[first + index]).wait()


def exchange_kernel(count, *refs):
    sources, targets = refs[:count], refs[count : 2 * count]
    send_sem, recv_sem = refs[2 * count :]
    greet()
    send_all(sources, targets, send_sem, recv_sem, 0)
    wait_all(targets, recv_sem, 0)
    wait_all(sources, send_sem, 0)


def exchange(arrays, collective_id):
    count = len(arrays)
    vmem = pl.BlockSpec(memory_space=pltpu.VMEM)
    return pl.pallas_call(
        functools.partial(exchange_kernel, count),
        out_shape=tuple(jax.ShapeDtypeStruct(array.shape, array.dtype) for array in arrays),
        in_specs=[vmem] * count,
        out_specs=(vmem,) * count,
        scratch_shapes=[pltpu.SemaphoreType.DMA((count,)), pltpu.SemaphoreType.DMA((count,))],
        compiler_params=pltpu.CompilerParams(collective_id=collective_id, has_side_effects=True),
        name="exchange" + str(collective_id),
    )(*arrays)


def combined(asked, parts, cluster):
    masked = jnp.where(asked == cluster, parts, lowest)
    upper = jnp.max(jnp.max(masked, axis=0), axis=0, keepdims=True)
    total = jnp.sum(jnp.sum(jnp.exp(masked - upper[None]), axis=0), axis=0, keepdims=True)
    return upper + jnp.log(total)


def turn_kernel(column_ref, asked_ref, mass_ref, u_ref, parts_ref, outgoing_ref, send_sem, recv_sem):
    greet()
    send_all([column_ref], [parts_ref], send_sem, recv_sem, 0)
    wait_all([parts_ref], recv_sem, 0)
    asked, parts = asked_ref[...], parts_ref[...]

    outgoing = jnp.zeros(parts.shape, jnp.float32)
    for cluster in range(mass_ref.shape[0]):
        row = mass_ref[cluster : cluster + 1, :] - combined(asked, parts, cluster)
        outgoing = jnp.where(asked == cluster, row[None], outgoing)
    outgoing_ref[...] = outgoing
    send_all([outgoing_ref], [u_ref], send_sem, recv_sem, 1)
    wait_all([u_ref], recv_sem, 1)
    wait_all([column_ref, outgoing_ref], send_sem, 0)


def finish_kernel(column_ref, asked_ref, level_ref, parts_ref, send_sem, recv_sem):
    greet()
    send_all([column_ref], [parts_ref], send_sem, recv_sem, 0)
    wait_all([parts_ref], recv_sem, 0)
    asked, parts = asked_ref[...], parts_ref[...]
    for cluster in range(level_ref.shape[0]):
        level_ref[cluster : cluster + 1, :] = combined(asked, parts, cluster)
    wait_all([column_ref], send_sem, 0)


def owner_call(kernel, out, scratch, collective_id, *operands):
    vmem = pl.BlockSpec(memory_space=pltpu.VMEM)
    return pl.pallas_call(
        kernel,
        out_shape=out,
        in_specs=[vmem] * len(operands),
        out_specs=vmem,
        scratch_shapes=scratch
        + [pltpu.SemaphoreType.DMA((2,)), pltpu.SemaphoreType.DMA((2,))],
        compiler_params=pltpu.CompilerParams(collective_id=collective_id, has_side_effects=True),
        name="owner" + str(collective_id),
    )(*operands)


def bias_rows(row, ones_first):
    high = row.astype(jnp.bfloat16).astype(jnp.float32)
    rest = row - high
    middle = rest.astype(jnp.bfloat16).astype(jnp.float32)
    low = rest - middle
    index = lax.broadcasted_iota(jnp.int32, (EXTRA, row.shape[1]), 0)
    where, other = (3, 0) if ones_first else (0, 3)
    ones = jnp.where((index >= other) & (index < other + 3), 1.0, 0.0)
    return jnp.where(
        index == where,
        high,
        jnp.where(index == where + 1, middle, jnp.where(index == where + 2, low, ones)),
    )


def split_rows(row):
    high = row.astype(jnp.bfloat16).astype(jnp.float32)
    index = lax.broadcasted_iota(jnp.int32, (16, row.shape[1]), 0)
    return jnp.where(index == 0, high, jnp.where(index == 1, row - high, 0.0)).astype(jnp.bfloat16)


def whole_max(array):
    return jnp.max(jnp.max(array, axis=0, keepdims=True), axis=1, keepdims=True)


def start_copy(source, target, sems, index, step):
    me = place()[0]
    peer, where = peer_of(step)
    pltpu.make_async_remote_copy(
        src_ref=source.at[peer],
        dst_ref=target.at[me],
        send_sem=sems[0].at[index],
        recv_sem=sems[1].at[index],
        device_id=where,
        device_id_type=MESH,
    ).start()


def plan_kernel(
    slots_ref, slot_row_ref, request_ref, source_ref, target_ref, mass_ref, target_mass_ref, coarse_ref,
    f_ref, g_ref, flag_ref,
    asked, asked_scalar, near, beta, tile_out, tiles, beta_out, betas, beta_next, columns, parts, columns_next, parts_next,
    left, right, kernel_store, weight, level_f, rows, local_sem, send_sem, recv_sem,
):
    me, devices, _ = place()
    clusters, features, points = source_ref.shape
    entries = slots_ref.shape[1]
    slots = devices * CAP
    sems = (send_sem, recv_sem)
    greet()
    send_all([request_ref], [asked], send_sem, recv_sem, 0)

    def prepare_source(cluster, carry):
        wide = source_ref[cluster].astype(jnp.float32)
        square = jnp.sum(wide * wide, axis=0, keepdims=True)
        stacked = jnp.concatenate([4.0 * wide, bias_rows(LIFT - 2.0 * square, False)], axis=0)
        left[cluster] = stacked.T.astype(jnp.bfloat16)
        return carry

    lax.fori_loop(0, clusters, prepare_source, 0, unroll=2)
    near[...] = 2.0 * coarse_ref[...] + target_mass_ref[...]
    wait_all([asked], recv_sem, 0)
    scalars = pltpu.make_async_copy(asked, asked_scalar, local_sem.at[0])
    scalars.start()
    scalars.wait()

    def serve(step, carry):
        peer = peer_of(step)[0]
        for entry in range(CAP):
            chosen = asked_scalar[peer, entry, 0]
            tile_out[peer, entry] = target_ref[chosen]
            beta_out[peer, pl.ds(entry, 1), :] = near[pl.ds(chosen, 1), :]
        start_copy(tile_out, tiles, sems, 1, step)
        start_copy(beta_out, betas, sems, 2, step)
        return carry

    lax.fori_loop(1, devices, serve, 0, unroll=1)
    for entry in range(CAP):
        chosen = asked_scalar[me, entry, 0]
        tiles[me, entry] = target_ref[chosen]
        betas[me, pl.ds(entry, 1), :] = near[pl.ds(chosen, 1), :]
    wait_all([betas], recv_sem, 2)
    wait_all([tiles], recv_sem, 1)

    def prepare_target(owner, carry):
        for entry in range(CAP):
            tile = tiles[owner, entry]
            wide = tile.astype(jnp.float32)
            square = jnp.sum(wide * wide, axis=0, keepdims=True)
            extra = bias_rows(LIFT - 2.0 * square, True).astype(jnp.bfloat16)
            right[owner * CAP + entry] = jnp.concatenate([tile, extra], axis=0)
        return carry

    lax.fori_loop(0, devices, prepare_target, 0, unroll=4)

    def set_weights(values):
        top = whole_max(values.reshape(slots, points))
        weight[...] = jnp.exp(values.reshape(slots, points) - top)
        return top

    def close_row(cluster, total, top):
        row = jnp.sum(total.T, axis=0, keepdims=True)
        level_f[pl.ds(cluster, 1), :] = row

    def build(cluster, carry):
        total = jnp.zeros((points, points), jnp.float32)
        for pair in range(entries // 2):
            chosen = [slots_ref[cluster, 2 * pair + lane] for lane in range(2)]
            rhs = jnp.concatenate([right[slot] for slot in chosen], axis=1)
            values = jnp.exp(jnp.dot(left[cluster], rhs, preferred_element_type=jnp.float32))
            kernel_store[cluster, :, pl.ds(pair * 2 * points, 2 * points)] = values.astype(jnp.bfloat16)
            for lane, slot in enumerate(chosen):
                total = total + values[:, lane * points : (lane + 1) * points] * weight[pl.ds(slot, 1), :]
        close_row(cluster, total, carry)
        return carry

    def forward(cluster, carry):
        total = jnp.zeros((points, points), jnp.float32)
        for entry in range(entries):
            values = kernel_store[cluster, :, pl.ds(entry * points, points)].astype(jnp.float32)
            total = total + values * weight[pl.ds(slots_ref[cluster, entry], 1), :]
        close_row(cluster, total, carry)
        return carry

    hot = jnp.where(
        slot_row_ref[...] == lax.broadcasted_iota(jnp.int32, (slots, clusters * entries), 0), 1.0, 0.0
    ).astype(jnp.bfloat16)

    def backward(top):
        sums = level_f[...]
        level = jnp.log(sums) + (top - 2.0 * LIFT)
        low = jnp.max(whole_max(jnp.where(sums >= FLOOR, 0.0, 1.0)), axis=0, keepdims=True)
        level_f[...] = level
        alpha = mass_ref[...] - level
        peak = whole_max(alpha)

        def visit(cluster, carry):
            lifted = jnp.exp(mass_ref[pl.ds(cluster, 1), :] - level_f[pl.ds(cluster, 1), :] - peak)
            products = jnp.dot(split_rows(lifted), kernel_store[cluster], preferred_element_type=jnp.float32)
            row = products[0:1] + products[1:2]
            for entry in range(entries):
                rows[pl.ds(cluster * entries + entry, 1), :] = row[:, entry * points : (entry + 1) * points]
            return carry

        lax.fori_loop(0, clusters, visit, 0)
        values = rows[...]
        high = values.astype(jnp.bfloat16)
        rest = values - high.astype(jnp.float32)
        middle = rest.astype(jnp.bfloat16)
        tail = (rest - middle.astype(jnp.float32)).astype(jnp.bfloat16)
        total = jnp.dot(hot, high, preferred_element_type=jnp.float32)
        total = total + jnp.dot(hot, middle, preferred_element_type=jnp.float32)
        total = total + jnp.dot(hot, tail, preferred_element_type=jnp.float32)
        low = jnp.maximum(low, whole_max(jnp.where(total >= FLOOR, 0.0, 1.0)))
        column = jnp.log(total) + (peak - 2.0 * LIFT)
        return jnp.where(low > 0.0, ALARM, column).reshape(devices, CAP, points)

    top = set_weights(betas[...])
    lax.fori_loop(0, clusters, build, 0)
    columns[...] = backward(top)
    send_all([columns], [parts], send_sem, recv_sem, 3)
    wait_all([parts], recv_sem, 3)
    for cluster in range(clusters):
        near[cluster : cluster + 1, :] = target_mass_ref[cluster : cluster + 1, :] - combined(
            asked[...], parts[...], cluster
        )

    def answer(step, carry):
        peer = peer_of(step)[0]
        for entry in range(CAP):
            beta_out[peer, pl.ds(entry, 1), :] = near[pl.ds(asked_scalar[peer, entry, 0], 1), :]
        start_copy(beta_out, beta_next, sems, 4, step)
        return carry

    wait_all([beta_out], send_sem, 2)
    lax.fori_loop(1, devices, answer, 0, unroll=1)
    for entry in range(CAP):
        beta_next[me, pl.ds(entry, 1), :] = near[pl.ds(asked_scalar[me, entry, 0], 1), :]
    wait_all([beta_next], recv_sem, 4)
    top = set_weights(beta_next[...])
    lax.fori_loop(0, clusters, forward, 0)
    columns_next[...] = backward(top)
    send_all([columns_next], [parts_next], send_sem, recv_sem, 5)
    f_ref[...] = -0.5 * level_f[...]
    wait_all([parts_next], recv_sem, 5)
    for cluster in range(clusters):
        g_ref[cluster : cluster + 1, :] = -0.5 * combined(asked[...], parts_next[...], cluster)
    alarm = jnp.maximum(parts[...].reshape(slots, points), parts_next[...].reshape(slots, points))
    flag_ref[...] = jnp.broadcast_to(
        whole_max(jnp.where(alarm < 1e30, 0.0, 1.0)), flag_ref.shape
    )
    wait_all([request_ref], send_sem, 0)
    wait_all([tile_out], send_sem, 1)
    wait_all([columns], send_sem, 3)
    wait_all([beta_out], send_sem, 4)
    wait_all([columns_next], send_sem, 5)


def plan_call(slot_list, request, source, target, mass, target_mass, coarse):
    devices = request.shape[0]
    clusters, features, points = source.shape
    entries = slot_list.shape[1]
    slots = devices * CAP
    depth = features + EXTRA
    vmem = pl.BlockSpec(memory_space=pltpu.VMEM)
    row_block = pltpu.VMEM((devices, CAP, points), jnp.float32)
    tile_block = pltpu.VMEM((devices, CAP, features, points), jnp.bfloat16)
    sems = pltpu.SemaphoreType.DMA((6,))
    return pl.pallas_call(
        plan_kernel,
        out_shape=(
            jax.ShapeDtypeStruct((clusters, points), jnp.float32),
            jax.ShapeDtypeStruct((clusters, points), jnp.float32),
            jax.ShapeDtypeStruct((8, points), jnp.float32),
        ),
        in_specs=[pl.BlockSpec(memory_space=pltpu.SMEM)] + [vmem] * 7,
        out_specs=(vmem, vmem, vmem),
        scratch_shapes=[
            pltpu.VMEM((devices, CAP, points), jnp.int32),
            pltpu.SMEM((devices, CAP, points), jnp.int32),
            pltpu.VMEM((clusters, points), jnp.float32),
            pltpu.VMEM((clusters, points), jnp.float32),
            tile_block, tile_block,
            row_block, row_block, row_block, row_block, row_block, row_block, row_block,
            pltpu.VMEM((clusters, points, depth), jnp.bfloat16),
            pltpu.VMEM((slots, depth, points), jnp.bfloat16),
            pltpu.VMEM((clusters, points, entries * points), jnp.bfloat16),
            pltpu.VMEM((slots, points), jnp.float32),
            pltpu.VMEM((clusters, points), jnp.float32),
            pltpu.VMEM((clusters * entries, points), jnp.float32),
            pltpu.SemaphoreType.DMA((1,)), sems, sems,
        ],
        compiler_params=pltpu.CompilerParams(
            collective_id=8, has_side_effects=True, vmem_limit_bytes=60 * 1024 * 1024
        ),
        name="plan",
    )(slot_list, slot_list.reshape(1, -1), request, source, target, mass, target_mass, coarse)


def careful(slot_list, request, source_points, target_points, source_mass, target_mass, coarse_potential):
    devices = request.shape[0]
    local_count, features, points = source_points.shape
    shape = (devices, CAP, points)
    (asked,) = exchange([request], 0)
    target_sq = squares(target_points)
    source_sq = squares(source_points)
    u = 2.0 * (coarse_potential - target_sq) + target_mass
    matches = asked[:, :, None, :] == jnp.arange(local_count, dtype=jnp.int32)[:, None]
    sending = jnp.sum(jnp.where(matches, u, 0.0), axis=2)
    tiles, received = exchange([target_points[asked[:, :, 0]], sending], 1)
    tiles = tiles.reshape(devices * CAP, features, points)
    row_shape = jax.ShapeDtypeStruct(shape, jnp.float32)
    level_shape = jax.ShapeDtypeStruct(target_mass.shape, jnp.float32)
    buffer = pltpu.VMEM(shape, jnp.float32)
    for sweep in range(ITERS):
        level, column = sweep_call(
            slot_list, source_points, source_mass, tiles, received.reshape(devices * CAP, points)
        )
        column = column.reshape(shape)
        if sweep < ITERS - 1:
            received = owner_call(
                turn_kernel, row_shape, [buffer, buffer], 2 + sweep, column, asked, target_mass
            )
    column_level = owner_call(finish_kernel, level_shape, [buffer], 1 + ITERS, column, asked)
    return (source_sq - 0.5 * level, target_sq - 0.5 * column_level)


def body(source_points, target_points, source_mass, target_mass, support, coarse_potential):
    devices = lax.axis_size(AXES)
    local_count, features, points = source_points.shape
    owner = support // local_count
    within = support % local_count
    flat_owner, flat_within = owner.reshape(-1), within.reshape(-1)
    named = flat_owner[None, :] == jnp.arange(devices, dtype=jnp.int32)[:, None]
    first = jnp.min(jnp.where(named, flat_within[None, :], local_count), axis=1)
    second = jnp.max(jnp.where(named, flat_within[None, :], -1), axis=1)
    request = jnp.stack([first, second], axis=1).astype(jnp.int32)
    request = jnp.broadcast_to(request[:, :, None], (devices, CAP, points))
    first_of = jnp.sum(jnp.where(named, first[:, None], 0), axis=0).reshape(owner.shape)
    slot_list = (owner * CAP + (within > first_of).astype(jnp.int32)).astype(jnp.int32)
    f, g, flag = plan_call(
        slot_list, request, source_points, target_points, source_mass, target_mass, coarse_potential
    )

    def again():
        return careful(
            slot_list, request, source_points, target_points, source_mass, target_mass, coarse_potential
        )

    return lax.cond(flag[0, 0] > 0.0, again, lambda: (f, g))


def solution(mesh):
    placed = (
        P(AXES, None, None),
        P(AXES, None, None),
        P(AXES, None),
        P(AXES, None),
        P(AXES, None),
        P(AXES, None),
    )
    return jax.shard_map(
        body,
        mesh=mesh,
        in_specs=placed,
        out_specs=(P(AXES, None), P(AXES, None)),
        check_vma=False,
    )
```

```python
import functools

import jax
import jax.numpy as jnp
from jax import lax
from jax.experimental import pallas as pl
from jax.experimental.pallas import tpu as pltpu
from jax.sharding import PartitionSpec as P

CAP = 2
EXTRA = 16
LIFT = 20.0
FLOOR = 1e-10
ALARM = 3e38
SENDS = 10
ITERS = 2
AXES = ("row", "col")
GROUP = 4
MESH = pl.DeviceIdType.MESH


epsilon = 0.5
lowest = -1e30


def squares(points):
    wide = points.astype(jnp.float32)
    return jnp.sum(wide * wide, axis=-2)


def pieces(row, depth):
    high = row.astype(jnp.bfloat16).astype(jnp.float32)
    rest = row - high
    middle = rest.astype(jnp.bfloat16).astype(jnp.float32)
    low = rest - middle
    index = lax.broadcasted_iota(jnp.int32, (depth, row.shape[1]), 0)
    return jnp.where(
        index == 0, high, jnp.where(index == 1, middle, jnp.where(index == 2, low, 0.0))
    )


def ones_rows(depth, points):
    index = lax.broadcasted_iota(jnp.int32, (depth, points), 0)
    return jnp.where(index < 3, 1.0, 0.0)


def fold(old_max, old_sum, scores):
    rows, lanes = scores.shape
    blocks = scores.reshape(rows // 8, 8, lanes)
    upper = jnp.maximum(old_max, jnp.max(blocks, axis=0))
    total = old_sum * jnp.exp(old_max - upper) + jnp.sum(jnp.exp(blocks - upper[None]), axis=0)
    return upper, total


def sweep_kernel(
    slots_ref, source_ref, mass_ref, tiles_ref, u_ref, row_ref, column_ref,
    tile_forward, tile_backward, run_max, run_sum,
):
    clusters, features, points = source_ref.shape
    slots = tiles_ref.shape[0]
    entries = slots_ref.shape[1]
    spare = tile_forward.shape[2] - features
    ones = ones_rows(spare, points)

    def prepare(slot, carry):
        tile = tiles_ref[slot].astype(jnp.float32)
        extra = pieces(u_ref[pl.ds(slot, 1), :], spare)
        tile_forward[slot] = jnp.concatenate([4.0 * tile, extra], axis=0).T.astype(jnp.bfloat16)
        tile_backward[slot] = jnp.concatenate([tile, ones], axis=0).astype(jnp.bfloat16)
        run_max[slot] = jnp.full((8, points), lowest, jnp.float32)
        run_sum[slot] = jnp.zeros((8, points), jnp.float32)
        return carry

    lax.fori_loop(0, slots, prepare, 0, unroll=8)

    def visit(cluster, carry):
        source = source_ref[cluster].astype(jnp.float32)
        right = jnp.concatenate([source, ones], axis=0).astype(jnp.bfloat16)

        def forward(step, state):
            lhs = jnp.concatenate(
                [tile_forward[slots_ref[cluster, step * GROUP + lane]] for lane in range(GROUP)],
                axis=0,
            )
            return fold(*state, jnp.dot(lhs, right, preferred_element_type=jnp.float32))

        start = (
            jnp.full((8, points), lowest, jnp.float32),
            jnp.zeros((8, points), jnp.float32),
        )
        upper, total = lax.fori_loop(0, entries // GROUP, forward, start, unroll=True)
        peak = jnp.max(upper, axis=0, keepdims=True)
        total = jnp.sum(total * jnp.exp(upper - peak), axis=0, keepdims=True)
        level = peak + jnp.log(total)
        row_ref[pl.ds(cluster, 1), :] = level
        extra = pieces(mass_ref[pl.ds(cluster, 1), :] - level, spare)
        left = jnp.concatenate([4.0 * source, extra], axis=0).T.astype(jnp.bfloat16)

        def backward(step, state):
            chosen = [slots_ref[cluster, step * GROUP + lane] for lane in range(GROUP)]
            held = [(run_max[slot], run_sum[slot]) for slot in chosen]
            rhs = jnp.concatenate([tile_backward[slot] for slot in chosen], axis=1)
            scores = jnp.dot(left, rhs, preferred_element_type=jnp.float32)
            fresh = [
                fold(*held[lane], scores[:, lane * points : (lane + 1) * points])
                for lane in range(GROUP)
            ]
            for slot, (new_max, new_sum) in zip(chosen, fresh):
                run_max[slot] = new_max
                run_sum[slot] = new_sum
            return state

        lax.fori_loop(0, entries // GROUP, backward, 0, unroll=True)
        return carry

    lax.fori_loop(0, clusters, visit, 0)
    upper = run_max[...]
    peak = jnp.max(upper, axis=1, keepdims=True)
    total = jnp.sum(run_sum[...] * jnp.exp(upper - peak), axis=1)
    column_ref[...] = peak[:, 0] + jnp.log(total)


def sweep_call(slot_list, source, mass, tiles, u):
    clusters, features, points = source.shape
    slots = tiles.shape[0]
    depth = 2 * features
    vmem = pl.BlockSpec(memory_space=pltpu.VMEM)
    pairs = clusters * slot_list.shape[1]
    return pl.pallas_call(
        sweep_kernel,
        out_shape=(
            jax.ShapeDtypeStruct((clusters, points), jnp.float32),
            jax.ShapeDtypeStruct((slots, points), jnp.float32),
        ),
        in_specs=[pl.BlockSpec(memory_space=pltpu.SMEM), vmem, vmem, vmem, vmem],
        out_specs=(vmem, vmem),
        scratch_shapes=[
            pltpu.VMEM((slots, points, depth), jnp.bfloat16),
            pltpu.VMEM((slots, depth, points), jnp.bfloat16),
            pltpu.VMEM((slots, 8, points), jnp.float32),
            pltpu.VMEM((slots, 8, points), jnp.float32),
        ],
        cost_estimate=pl.CostEstimate(
            flops=4 * pairs * points * points * depth,
            transcendentals=2 * pairs * points * points,
            bytes_accessed=2 * slots * features * points,
        ),
        name="sweep",
    )(slot_list, source, mass, tiles, u)


def place():
    rows, columns = lax.axis_size("row"), lax.axis_size("col")
    return lax.axis_index("row") * columns + lax.axis_index("col"), rows * columns, columns


def peer_of(step):
    me, devices, columns = place()
    peer = lax.rem(me + step, devices)
    return peer, (lax.div(peer, columns), lax.rem(peer, columns))


def greet():
    devices = place()[1]
    barrier = pltpu.get_barrier_semaphore()

    def signal(step, carry):
        pl.semaphore_signal(barrier, inc=1, device_id=peer_of(step)[1], device_id_type=MESH)
        return carry

    lax.fori_loop(1, devices, signal, 0, unroll=8)
    pl.semaphore_wait(barrier, devices - 1)


def send_all(sources, targets, send_sem, recv_sem, first):
    me, devices, _ = place()

    def send(step, carry):
        peer, where = peer_of(step)
        for index, (source, target) in enumerate(zip(sources, targets)):
            pltpu.make_async_remote_copy(
                src_ref=source.at[peer],
                dst_ref=target.at[me],
                send_sem=send_sem.at[first + index],
                recv_sem=recv_sem.at[first + index],
                device_id=where,
                device_id_type=MESH,
            ).start()
        return carry

    lax.fori_loop(1, devices, send, 0, unroll=8)
    for source, target in zip(sources, targets):
        target[me] = source[me]


def wait_all(refs, sems, first):
    devices = place()[1]
    for index, ref in enumerate(refs):
        blocks = ref.at[pl.ds(0, devices - 1)]
        pltpu.make_async_copy(blocks, blocks, sems.at[first + index]).wait()


def exchange_kernel(count, *refs):
    sources, targets = refs[:count], refs[count : 2 * count]
    send_sem, recv_sem = refs[2 * count :]
    greet()
    send_all(sources, targets, send_sem, recv_sem, 0)
    wait_all(targets, recv_sem, 0)
    wait_all(sources, send_sem, 0)


def exchange(arrays, collective_id):
    count = len(arrays)
    vmem = pl.BlockSpec(memory_space=pltpu.VMEM)
    return pl.pallas_call(
        functools.partial(exchange_kernel, count),
        out_shape=tuple(jax.ShapeDtypeStruct(array.shape, array.dtype) for array in arrays),
        in_specs=[vmem] * count,
        out_specs=(vmem,) * count,
        scratch_shapes=[pltpu.SemaphoreType.DMA((count,)), pltpu.SemaphoreType.DMA((count,))],
        compiler_params=pltpu.CompilerParams(collective_id=collective_id, has_side_effects=True),
        name="exchange" + str(collective_id),
    )(*arrays)


def combined(asked, parts, cluster):
    masked = jnp.where(asked == cluster, parts, lowest)
    upper = jnp.max(jnp.max(masked, axis=0), axis=0, keepdims=True)
    total = jnp.sum(jnp.sum(jnp.exp(masked - upper[None]), axis=0), axis=0, keepdims=True)
    return upper + jnp.log(total)


def turn_kernel(column_ref, asked_ref, mass_ref, u_ref, parts_ref, outgoing_ref, send_sem, recv_sem):
    greet()
    send_all([column_ref], [parts_ref], send_sem, recv_sem, 0)
    wait_all([parts_ref], recv_sem, 0)
    asked, parts = asked_ref[...], parts_ref[...]

    outgoing = jnp.zeros(parts.shape, jnp.float32)
    for cluster in range(mass_ref.shape[0]):
        row = mass_ref[cluster : cluster + 1, :] - combined(asked, parts, cluster)
        outgoing = jnp.where(asked == cluster, row[None], outgoing)
    outgoing_ref[...] = outgoing
    send_all([outgoing_ref], [u_ref], send_sem, recv_sem, 1)
    wait_all([u_ref], recv_sem, 1)
    wait_all([column_ref, outgoing_ref], send_sem, 0)


def finish_kernel(column_ref, asked_ref, level_ref, parts_ref, send_sem, recv_sem):
    greet()
    send_all([column_ref], [parts_ref], send_sem, recv_sem, 0)
    wait_all([parts_ref], recv_sem, 0)
    asked, parts = asked_ref[...], parts_ref[...]
    for cluster in range(level_ref.shape[0]):
        level_ref[cluster : cluster + 1, :] = combined(asked, parts, cluster)
    wait_all([column_ref], send_sem, 0)


def owner_call(kernel, out, scratch, collective_id, *operands):
    vmem = pl.BlockSpec(memory_space=pltpu.VMEM)
    return pl.pallas_call(
        kernel,
        out_shape=out,
        in_specs=[vmem] * len(operands),
        out_specs=vmem,
        scratch_shapes=scratch
        + [pltpu.SemaphoreType.DMA((2,)), pltpu.SemaphoreType.DMA((2,))],
        compiler_params=pltpu.CompilerParams(collective_id=collective_id, has_side_effects=True),
        name="owner" + str(collective_id),
    )(*operands)


def bias_rows(row, ones_first):
    high = row.astype(jnp.bfloat16).astype(jnp.float32)
    rest = row - high
    middle = rest.astype(jnp.bfloat16).astype(jnp.float32)
    low = rest - middle
    index = lax.broadcasted_iota(jnp.int32, (EXTRA, row.shape[1]), 0)
    where, other = (3, 0) if ones_first else (0, 3)
    ones = jnp.where((index >= other) & (index < other + 3), 1.0, 0.0)
    return jnp.where(
        index == where,
        high,
        jnp.where(index == where + 1, middle, jnp.where(index == where + 2, low, ones)),
    )


def split_rows(row):
    high = row.astype(jnp.bfloat16).astype(jnp.float32)
    index = lax.broadcasted_iota(jnp.int32, (16, row.shape[1]), 0)
    return jnp.where(index == 0, high, jnp.where(index == 1, row - high, 0.0)).astype(jnp.bfloat16)


def whole_max(array):
    return jnp.max(jnp.max(array, axis=0, keepdims=True), axis=1, keepdims=True)


def halves():
    me, devices, columns = place()
    half = devices // 2
    side = lax.div(me, half)
    return side, me - side * half, half, columns


def block_of(step):
    side, mine, half, columns = halves()
    other = lax.div(step, half)
    near = lax.rem(mine + lax.rem(step, half), half)
    device = lax.rem(side + other, 2) * half + near
    return other * half + near, near, (lax.div(device, columns), lax.rem(device, columns))


def start_copy(source, target, sems, index, where):
    pltpu.make_async_remote_copy(
        src_ref=source,
        dst_ref=target,
        send_sem=sems[0].at[index],
        recv_sem=sems[1].at[index],
        device_id=where,
        device_id_type=MESH,
    ).start()


def wait_blocks(ref, count, sem):
    blocks = ref if count is None else ref.at[pl.ds(0, count)]
    pltpu.make_async_copy(blocks, blocks, sem).wait()


def plan_kernel(
    support_ref, names_ref, source_ref, target_ref, mass_ref, target_mass_ref, coarse_ref,
    f_ref, g_ref, flag_ref,
    codes, codes_scalar, asked_near, asked_far, asked_scalar, slots_ref,
    near, mate, mate_near, tile_out, mate_out, tiles, mate_tiles,
    beta_out, mate_beta_out, betas, mate_betas, beta_next_out, beta_next,
    columns, parts, columns_next, parts_next,
    left, right, store_even, store_odd, weight, sums, level_f, peaks, lifted, hot, rows,
    local_sem, send_sem, recv_sem,
):
    me, devices, _ = place()
    side, mine, half, _ = halves()
    clusters, features, points = source_ref.shape
    entries = support_ref.shape[1]
    slots = devices * CAP
    sems = (send_sem, recv_sem)
    barrier = pltpu.get_barrier_semaphore()

    def signal(step, carry):
        pl.semaphore_signal(barrier, inc=1, device_id=block_of(step)[2], device_id_type=MESH)
        return carry

    lax.fori_loop(1, devices, signal, 0, unroll=8)

    block = lax.broadcasted_iota(jnp.int32, (devices, entries), 0)
    far = jnp.where(block >= half, 1, 0)
    owner_of_block = jnp.where(far == 1, 1 - side, side) * half + block - far * half
    first = jnp.full((devices, entries), clusters, jnp.int32)
    second = jnp.full((devices, entries), -1, jnp.int32)
    for cluster in range(clusters):
        name = names_ref[cluster : cluster + 1, :]
        within = name - owner_of_block * clusters
        named = (within >= 0) & (within < clusters)
        first = jnp.minimum(first, jnp.where(named, within, clusters))
        second = jnp.maximum(second, jnp.where(named, within, -1))
    first = jnp.min(first, axis=1, keepdims=True)
    second = jnp.max(second, axis=1, keepdims=True)
    own = jnp.broadcast_to(first * clusters + second, (devices, points))
    swapped = jnp.concatenate([own[half:], own[:half]], axis=0)
    lane = lax.broadcasted_iota(jnp.int32, (devices, points), 1)
    codes[...] = jnp.where(lane < points // 2, own, swapped).reshape(devices, 1, points)
    slot_block = lax.broadcasted_iota(jnp.int32, (slots, entries), 0)
    pair_first = jnp.broadcast_to(first.reshape(devices, 1, 1), (devices, CAP, entries)).reshape(slots, entries)
    pair_second = jnp.broadcast_to(second.reshape(devices, 1, 1), (devices, CAP, entries)).reshape(slots, entries)
    slot_device = lax.div(slot_block, CAP)
    slot_far = jnp.where(slot_device >= half, 1, 0)
    slot_owner = jnp.where(slot_far == 1, 1 - side, side) * half + slot_device - slot_far * half
    slot_name = slot_owner * clusters + jnp.where(lax.rem(slot_block, CAP) == 0, pair_first, pair_second)
    near[...] = 2.0 * coarse_ref[...] + target_mass_ref[...]
    pl.semaphore_wait(barrier, devices - 1)

    def ask(step, carry):
        to, _, where = block_of(step)
        start_copy(codes.at[to], asked_near.at[mine], sems, 0, where)
        return carry

    def ask_far(step, carry):
        to, _, where = block_of(step)
        start_copy(codes.at[to], asked_far.at[mine], sems, 1, where)
        return carry

    lax.fori_loop(1, half, ask, 0, unroll=5)
    mate_where = block_of(half)[2]
    start_copy(target_ref, mate, sems, 2, mate_where)
    start_copy(near, mate_near, sems, 3, mate_where)
    lax.fori_loop(half, devices, ask_far, 0, unroll=8)
    local = pltpu.make_async_copy(codes, codes_scalar, local_sem.at[0])
    local.start()

    def prepare_source(cluster, carry):
        wide = source_ref[cluster].astype(jnp.float32)
        square = jnp.sum(wide * wide, axis=0, keepdims=True)
        stacked = jnp.concatenate([4.0 * wide, bias_rows(LIFT - 2.0 * square, False)], axis=0)
        left[cluster] = stacked.T.astype(jnp.bfloat16)
        return carry

    local.wait()
    asked_near[mine] = codes[mine]
    wait_blocks(asked_near, half - 1, recv_sem.at[0])
    scalars = pltpu.make_async_copy(asked_near, asked_scalar, local_sem.at[1])
    scalars.start()
    scalars.wait()

    def serve(origin, origin_near, tile_to, beta_to, tile_in, beta_in, lane, index):
        def one(step, carry):
            to, near_index, where = block_of(step)
            code = asked_scalar[near_index, 0, lane]
            chosen = lax.div(code, clusters)
            for entry, pick in enumerate((chosen, code - chosen * clusters)):
                tile_to[near_index, entry] = origin[pick]
                beta_to[near_index, pl.ds(entry, 1), :] = origin_near[pl.ds(pick, 1), :]
            start_copy(tile_to.at[near_index], tile_in.at[mine], sems, index, where)
            start_copy(beta_to.at[near_index], beta_in.at[mine], sems, index + 1, where)
            return carry

        lax.fori_loop(1, half, one, 0)
        code = asked_scalar[mine, 0, lane]
        chosen = lax.div(code, clusters)
        for entry, pick in enumerate((chosen, code - chosen * clusters)):
            tile_in[mine, entry] = origin[pick]
            beta_in[mine, pl.ds(entry, 1), :] = origin_near[pl.ds(pick, 1), :]

    serve(target_ref, near, tile_out, beta_out, tiles, betas, 0, 4)
    lax.fori_loop(0, clusters, prepare_source, 0, unroll=2)

    def place_slots(cluster, carry):
        for entry in range(entries):
            name = support_ref[cluster, entry]
            owner = lax.div(name, clusters)
            owner_side = lax.div(owner, half)
            to = lax.rem(owner_side + side, 2) * half + owner - owner_side * half
            late = name - owner * clusters > lax.div(codes_scalar[to, 0, 0], clusters)
            slots_ref[cluster, entry] = to * CAP + late.astype(jnp.int32)
        return carry

    lax.fori_loop(0, clusters, place_slots, 0)
    for cluster in range(clusters):
        hot[:, cluster * entries : (cluster + 1) * entries] = jnp.where(
            names_ref[cluster : cluster + 1, :] == slot_name, 1.0, 0.0
        )
    wait_blocks(mate, None, recv_sem.at[2])
    wait_blocks(mate_near, None, recv_sem.at[3])
    serve(mate, mate_near, mate_out, mate_beta_out, mate_tiles, mate_betas, points // 2, 6)

    def prepare_target(source, offset):
        def one(owner, carry):
            for entry in range(CAP):
                tile = source[owner, entry]
                wide = tile.astype(jnp.float32)
                square = jnp.sum(wide * wide, axis=0, keepdims=True)
                extra = bias_rows(LIFT - 2.0 * square, True).astype(jnp.bfloat16)
                right[offset + owner * CAP + entry] = jnp.concatenate([tile, extra], axis=0)
            return carry

        lax.fori_loop(0, half, one, 0, unroll=4)

    wait_blocks(betas, half - 1, recv_sem.at[5])
    wait_blocks(tiles, half - 1, recv_sem.at[4])
    prepare_target(tiles, 0)
    wait_blocks(mate_betas, half - 1, recv_sem.at[7])
    wait_blocks(mate_tiles, half - 1, recv_sem.at[6])
    prepare_target(mate_tiles, half * CAP)
    wait_blocks(asked_far, half, recv_sem.at[1])
    asked_own = jnp.concatenate([asked_near[...], asked_far[...]], axis=0)[:, :, 0:1]
    asked_code = jnp.broadcast_to(asked_own, (devices, CAP, points))
    asked_first = lax.div(asked_code, clusters)
    asked = jnp.where(
        lax.broadcasted_iota(jnp.int32, (devices, CAP, points), 1) == 0,
        asked_first,
        asked_code - asked_first * clusters,
    )

    def set_weights(values):
        top = whole_max(values)
        weight[...] = jnp.exp(values - top)
        return top

    def close(cluster, total, top):
        row = jnp.sum(total.T, axis=0, keepdims=True)
        level = jnp.log(row) + (top - 2.0 * LIFT)
        alpha = mass_ref[pl.ds(cluster, 1), :] - level
        peak = jnp.max(alpha, axis=1, keepdims=True)
        sums[pl.ds(cluster, 1), :] = row
        level_f[pl.ds(cluster, 1), :] = level
        peaks[pl.ds(cluster, 1), :] = jnp.broadcast_to(peak, (1, points))
        lifted[cluster] = split_rows(jnp.exp(alpha - peak))

    def build(cluster, store, index, pair, total):
        chosen = [slots_ref[cluster, 2 * pair + lane] for lane in range(2)]
        rhs = jnp.concatenate([right[slot] for slot in chosen], axis=1)
        values = jnp.exp(jnp.dot(left[cluster], rhs, preferred_element_type=jnp.float32))
        store[index, :, pl.ds(pair * 2 * points, 2 * points)] = values.astype(jnp.bfloat16)
        for lane, slot in enumerate(chosen):
            total = total + values[:, lane * points : (lane + 1) * points] * weight[pl.ds(slot, 1), :]
        return total

    def forward(cluster, store, index, pair, total):
        for lane in range(2):
            entry = 2 * pair + lane
            values = store[index, :, pl.ds(entry * points, points)].astype(jnp.float32)
            total = total + values * weight[pl.ds(slots_ref[cluster, entry], 1), :]
        return total

    def backward(cluster, store, index, pair):
        products = jnp.dot(
            lifted[cluster],
            store[index, :, pl.ds(pair * 2 * points, 2 * points)],
            preferred_element_type=jnp.float32,
        )
        row = products[0:1] + products[1:2]
        for lane in range(2):
            rows[pl.ds(cluster * entries + 2 * pair + lane, 1), :] = row[:, lane * points : (lane + 1) * points]

    def sweep(make, top):
        def mixed(cluster, store, index, before, old_store, old_index):
            total = jnp.zeros((points, points), jnp.float32)
            for pair in range(entries // 2):
                if before is not None:
                    backward(before, old_store, old_index, pair)
                if cluster is not None:
                    total = make(cluster, store, index, pair, total)
            if cluster is not None:
                close(cluster, total, top)

        def both(index, carry):
            mixed(2 * index + 1, store_odd, index, 2 * index, store_even, index)
            mixed(2 * index + 2, store_even, index + 1, 2 * index + 1, store_odd, index)
            return carry

        last = clusters // 2 - 1
        mixed(0, store_even, 0, None, None, None)
        lax.fori_loop(0, last, both, 0)
        mixed(clusters - 1, store_odd, last, clusters - 2, store_even, last)
        mixed(None, None, None, clusters - 1, store_odd, last)
        peak = whole_max(peaks[...])
        scale = jnp.exp(peaks[...] - peak)
        total = jnp.zeros((slots, points), jnp.float32)
        values = jnp.concatenate(
            [
                rows[pl.ds(cluster * entries, entries), :] * scale[cluster : cluster + 1, :]
                for cluster in range(clusters)
            ],
            axis=0,
        )
        choice = hot[...].astype(jnp.bfloat16)
        for _ in range(3):
            piece = values.astype(jnp.bfloat16)
            total = total + jnp.dot(choice, piece, preferred_element_type=jnp.float32)
            values = values - piece.astype(jnp.float32)
        low = jnp.maximum(
            whole_max(jnp.where(sums[...] >= FLOOR, 0.0, 1.0)), whole_max(jnp.where(total >= FLOOR, 0.0, 1.0))
        )
        column = jnp.log(total) + (peak - 2.0 * LIFT)
        return jnp.where(low > 0.0, ALARM, column).reshape(devices, CAP, points)

    def return_columns(source, target, index):
        def one(step, carry):
            to, near_index, where = block_of(step)
            landing = lax.div(to, half) * half + mine
            start_copy(source.at[to], target.at[landing], sems, index, where)
            return carry

        lax.fori_loop(1, devices, one, 0, unroll=8)
        target[mine] = source[mine]
        wait_blocks(target, devices - 1, recv_sem.at[index])

    start = jnp.concatenate([betas[...], mate_betas[...]], axis=0).reshape(slots, points)
    columns[...] = sweep(build, set_weights(start))
    return_columns(columns, parts, 8)
    for cluster in range(clusters):
        near_row = target_mass_ref[cluster : cluster + 1, :] - combined(asked, parts[...], cluster)
        beta_next_out[...] = jnp.where(asked == cluster, near_row[None], beta_next_out[...] if cluster else 0.0)
    return_columns(beta_next_out, beta_next, 9)
    columns_next[...] = sweep(forward, set_weights(beta_next[...].reshape(slots, points)))
    f_ref[...] = level_f[...]
    return_columns(columns_next, parts_next, 10)
    for cluster in range(clusters):
        g_ref[cluster : cluster + 1, :] = combined(asked, parts_next[...], cluster)
    alarm = jnp.maximum(parts[...].reshape(slots, points), parts_next[...].reshape(slots, points))
    flag_ref[...] = jnp.broadcast_to(whole_max(jnp.where(alarm < 1e30, 0.0, 1.0)), flag_ref.shape)
    wait_blocks(codes, half - 1, send_sem.at[0])
    wait_blocks(codes, half, send_sem.at[1])
    wait_blocks(mate, None, send_sem.at[2])
    wait_blocks(near, None, send_sem.at[3])
    wait_blocks(tile_out, half - 1, send_sem.at[4])
    wait_blocks(beta_out, half - 1, send_sem.at[5])
    wait_blocks(mate_out, half - 1, send_sem.at[6])
    wait_blocks(mate_beta_out, half - 1, send_sem.at[7])
    wait_blocks(columns, devices - 1, send_sem.at[8])
    wait_blocks(beta_next_out, devices - 1, send_sem.at[9])
    wait_blocks(columns_next, devices - 1, send_sem.at[10])


def plan_call(support, source, target, mass, target_mass, coarse):
    devices = lax.axis_size(AXES)
    clusters, features, points = source.shape
    entries = support.shape[1]
    slots = devices * CAP
    half = devices // 2
    depth = features + EXTRA
    vmem = pl.BlockSpec(memory_space=pltpu.VMEM)
    level = jax.ShapeDtypeStruct((clusters, points), jnp.float32)
    levels = pltpu.VMEM((clusters, points), jnp.float32)
    row_block = pltpu.VMEM((devices, CAP, points), jnp.float32)
    half_row = pltpu.VMEM((half, CAP, points), jnp.float32)
    half_tile = pltpu.VMEM((half, CAP, features, points), jnp.bfloat16)
    half_code = pltpu.VMEM((half, 1, points), jnp.int32)
    kernel_block = pltpu.VMEM((clusters // 2, points, entries * points), jnp.bfloat16)
    sems = pltpu.SemaphoreType.DMA((11,))
    return pl.pallas_call(
        plan_kernel,
        out_shape=(level, level, jax.ShapeDtypeStruct((8, points), jnp.float32)),
        in_specs=[pl.BlockSpec(memory_space=pltpu.SMEM)] + [vmem] * 6,
        out_specs=(vmem, vmem, vmem),
        scratch_shapes=[
            pltpu.VMEM((devices, 1, points), jnp.int32),
            pltpu.SMEM((devices, 1, points), jnp.int32),
            half_code,
            half_code,
            pltpu.SMEM((half, 1, points), jnp.int32),
            pltpu.SMEM((clusters, entries), jnp.int32),
            levels,
            pltpu.VMEM((clusters, features, points), jnp.bfloat16),
            levels,
            half_tile, half_tile, half_tile, half_tile,
            half_row, half_row, half_row, half_row,
            row_block, row_block, row_block, row_block, row_block, row_block,
            pltpu.VMEM((clusters, points, depth), jnp.bfloat16),
            pltpu.VMEM((slots, depth, points), jnp.bfloat16),
            kernel_block, kernel_block,
            pltpu.VMEM((slots, points), jnp.float32),
            levels, levels, levels,
            pltpu.VMEM((clusters, 16, points), jnp.bfloat16),
            pltpu.VMEM((slots, clusters * entries), jnp.float32),
            pltpu.VMEM((clusters * entries, points), jnp.float32),
            pltpu.SemaphoreType.DMA((2,)), sems, sems,
        ],
        compiler_params=pltpu.CompilerParams(
            collective_id=8, has_side_effects=True, vmem_limit_bytes=60 * 1024 * 1024
        ),
        name="plan",
    )(support, support, source, target, mass, target_mass, coarse)


def careful(source_points, target_points, source_mass, target_mass, support, coarse_potential):
    devices = lax.axis_size(AXES)
    local_count, features, points = source_points.shape
    owner = support // local_count
    within = support % local_count
    flat_owner, flat_within = owner.reshape(-1), within.reshape(-1)
    named = flat_owner[None, :] == jnp.arange(devices, dtype=jnp.int32)[:, None]
    first = jnp.min(jnp.where(named, flat_within[None, :], local_count), axis=1)
    second = jnp.max(jnp.where(named, flat_within[None, :], -1), axis=1)
    request = jnp.stack([first, second], axis=1).astype(jnp.int32)
    shape = (devices, CAP, points)
    (asked,) = exchange([jnp.broadcast_to(request[:, :, None], shape)], 0)
    first_of = jnp.sum(jnp.where(named, first[:, None], 0), axis=0).reshape(owner.shape)
    slot_list = (owner * CAP + (within > first_of).astype(jnp.int32)).astype(jnp.int32)

    target_sq = squares(target_points)
    source_sq = squares(source_points)
    u = 2.0 * (coarse_potential - target_sq) + target_mass
    matches = asked[:, :, None, :] == jnp.arange(local_count, dtype=jnp.int32)[:, None]
    sending = jnp.sum(jnp.where(matches, u, 0.0), axis=2)
    tiles, received = exchange([target_points[asked[:, :, 0]], sending], 1)
    tiles = tiles.reshape(devices * CAP, features, points)
    row_shape = jax.ShapeDtypeStruct(shape, jnp.float32)
    level_shape = jax.ShapeDtypeStruct(target_mass.shape, jnp.float32)
    buffer = pltpu.VMEM(shape, jnp.float32)
    for sweep in range(ITERS):
        level, column = sweep_call(
            slot_list, source_points, source_mass, tiles, received.reshape(devices * CAP, points)
        )
        column = column.reshape(shape)
        if sweep < ITERS - 1:
            received = owner_call(
                turn_kernel, row_shape, [buffer, buffer], 2 + sweep, column, asked, target_mass
            )
    column_level = owner_call(finish_kernel, level_shape, [buffer], 1 + ITERS, column, asked)
    return level - 2.0 * source_sq, column_level - 2.0 * target_sq


def body(source_points, target_points, source_mass, target_mass, support, coarse_potential):
    f, g, flag = plan_call(
        support, source_points, target_points, source_mass, target_mass, coarse_potential
    )

    def again():
        return careful(
            source_points, target_points, source_mass, target_mass, support, coarse_potential
        )

    f, g = lax.cond(flag[0, 0] > 0.0, again, lambda: (f, g))
    return -0.5 * f, -0.5 * g


def solution(mesh):
    placed = (
        P(AXES, None, None),
        P(AXES, None, None),
        P(AXES, None),
        P(AXES, None),
        P(AXES, None),
        P(AXES, None),
    )
    return jax.shard_map(
        body,
        mesh=mesh,
        in_specs=placed,
        out_specs=(P(AXES, None), P(AXES, None)),
        check_vma=False,
    )
```

```python
import functools

import jax
import jax.numpy as jnp
from jax import lax
from jax.experimental import pallas as pl
from jax.experimental.pallas import tpu as pltpu
from jax.sharding import PartitionSpec as P

CAP = 2
EXTRA = 16
LIFT = 20.0
FLOOR = 1e-10
ALARM = 3e38
ROOM = 17 * 1024 * 1024
TOGETHER = 2
EARLY = 3
CHUNKS = 2
RELAY = 11
PASS = RELAY + CHUNKS
LOGICAL = pl.DeviceIdType.LOGICAL
ITERS = 2
AXES = ("row", "col")
GROUP = 4
MESH = pl.DeviceIdType.MESH


epsilon = 0.5
lowest = -1e30


def squares(points):
    wide = points.astype(jnp.float32)
    return jnp.sum(wide * wide, axis=-2)


def pieces(row, depth):
    high = row.astype(jnp.bfloat16).astype(jnp.float32)
    rest = row - high
    middle = rest.astype(jnp.bfloat16).astype(jnp.float32)
    low = rest - middle
    index = lax.broadcasted_iota(jnp.int32, (depth, row.shape[1]), 0)
    return jnp.where(
        index == 0, high, jnp.where(index == 1, middle, jnp.where(index == 2, low, 0.0))
    )


def ones_rows(depth, points):
    index = lax.broadcasted_iota(jnp.int32, (depth, points), 0)
    return jnp.where(index < 3, 1.0, 0.0)


def fold(old_max, old_sum, scores):
    rows, lanes = scores.shape
    blocks = scores.reshape(rows // 8, 8, lanes)
    upper = jnp.maximum(old_max, jnp.max(blocks, axis=0))
    total = old_sum * jnp.exp(old_max - upper) + jnp.sum(jnp.exp(blocks - upper[None]), axis=0)
    return upper, total


def sweep_kernel(
    slots_ref, source_ref, mass_ref, tiles_ref, u_ref, row_ref, column_ref,
    tile_forward, tile_backward, run_max, run_sum,
):
    clusters, features, points = source_ref.shape
    slots = tiles_ref.shape[0]
    entries = slots_ref.shape[1]
    spare = tile_forward.shape[2] - features
    ones = ones_rows(spare, points)

    def prepare(slot, carry):
        tile = tiles_ref[slot].astype(jnp.float32)
        extra = pieces(u_ref[pl.ds(slot, 1), :], spare)
        tile_forward[slot] = jnp.concatenate([4.0 * tile, extra], axis=0).T.astype(jnp.bfloat16)
        tile_backward[slot] = jnp.concatenate([tile, ones], axis=0).astype(jnp.bfloat16)
        run_max[slot] = jnp.full((8, points), lowest, jnp.float32)
        run_sum[slot] = jnp.zeros((8, points), jnp.float32)
        return carry

    lax.fori_loop(0, slots, prepare, 0, unroll=8)

    def visit(cluster, carry):
        source = source_ref[cluster].astype(jnp.float32)
        right = jnp.concatenate([source, ones], axis=0).astype(jnp.bfloat16)

        def forward(step, state):
            lhs = jnp.concatenate(
                [tile_forward[slots_ref[cluster, step * GROUP + lane]] for lane in range(GROUP)],
                axis=0,
            )
            return fold(*state, jnp.dot(lhs, right, preferred_element_type=jnp.float32))

        start = (
            jnp.full((8, points), lowest, jnp.float32),
            jnp.zeros((8, points), jnp.float32),
        )
        upper, total = lax.fori_loop(0, entries // GROUP, forward, start, unroll=True)
        peak = jnp.max(upper, axis=0, keepdims=True)
        total = jnp.sum(total * jnp.exp(upper - peak), axis=0, keepdims=True)
        level = peak + jnp.log(total)
        row_ref[pl.ds(cluster, 1), :] = level
        extra = pieces(mass_ref[pl.ds(cluster, 1), :] - level, spare)
        left = jnp.concatenate([4.0 * source, extra], axis=0).T.astype(jnp.bfloat16)

        def backward(step, state):
            chosen = [slots_ref[cluster, step * GROUP + lane] for lane in range(GROUP)]
            held = [(run_max[slot], run_sum[slot]) for slot in chosen]
            rhs = jnp.concatenate([tile_backward[slot] for slot in chosen], axis=1)
            scores = jnp.dot(left, rhs, preferred_element_type=jnp.float32)
            fresh = [
                fold(*held[lane], scores[:, lane * points : (lane + 1) * points])
                for lane in range(GROUP)
            ]
            for slot, (new_max, new_sum) in zip(chosen, fresh):
                run_max[slot] = new_max
                run_sum[slot] = new_sum
            return state

        lax.fori_loop(0, entries // GROUP, backward, 0, unroll=True)
        return carry

    lax.fori_loop(0, clusters, visit, 0)
    upper = run_max[...]
    peak = jnp.max(upper, axis=1, keepdims=True)
    total = jnp.sum(run_sum[...] * jnp.exp(upper - peak), axis=1)
    column_ref[...] = peak[:, 0] + jnp.log(total)


def sweep_call(slot_list, source, mass, tiles, u):
    clusters, features, points = source.shape
    slots = tiles.shape[0]
    depth = 2 * features
    vmem = pl.BlockSpec(memory_space=pltpu.VMEM)
    pairs = clusters * slot_list.shape[1]
    return pl.pallas_call(
        sweep_kernel,
        out_shape=(
            jax.ShapeDtypeStruct((clusters, points), jnp.float32),
            jax.ShapeDtypeStruct((slots, points), jnp.float32),
        ),
        in_specs=[pl.BlockSpec(memory_space=pltpu.SMEM), vmem, vmem, vmem, vmem],
        out_specs=(vmem, vmem),
        scratch_shapes=[
            pltpu.VMEM((slots, points, depth), jnp.bfloat16),
            pltpu.VMEM((slots, depth, points), jnp.bfloat16),
            pltpu.VMEM((slots, 8, points), jnp.float32),
            pltpu.VMEM((slots, 8, points), jnp.float32),
        ],
        cost_estimate=pl.CostEstimate(
            flops=4 * pairs * points * points * depth,
            transcendentals=2 * pairs * points * points,
            bytes_accessed=2 * slots * features * points,
        ),
        name="sweep",
    )(slot_list, source, mass, tiles, u)


def place():
    rows, columns = lax.axis_size("row"), lax.axis_size("col")
    return lax.axis_index("row") * columns + lax.axis_index("col"), rows * columns, columns


def peer_of(step):
    me, devices, columns = place()
    peer = lax.rem(me + step, devices)
    return peer, (lax.div(peer, columns), lax.rem(peer, columns))


def greet():
    devices = place()[1]
    barrier = pltpu.get_barrier_semaphore()

    def signal(step, carry):
        pl.semaphore_signal(barrier, inc=1, device_id=peer_of(step)[1], device_id_type=MESH)
        return carry

    lax.fori_loop(1, devices, signal, 0, unroll=8)
    pl.semaphore_wait(barrier, devices - 1)


def send_all(sources, targets, send_sem, recv_sem, first):
    me, devices, _ = place()

    def send(step, carry):
        peer, where = peer_of(step)
        for index, (source, target) in enumerate(zip(sources, targets)):
            pltpu.make_async_remote_copy(
                src_ref=source.at[peer],
                dst_ref=target.at[me],
                send_sem=send_sem.at[first + index],
                recv_sem=recv_sem.at[first + index],
                device_id=where,
                device_id_type=MESH,
            ).start()
        return carry

    lax.fori_loop(1, devices, send, 0, unroll=8)
    for source, target in zip(sources, targets):
        target[me] = source[me]


def wait_all(refs, sems, first):
    devices = place()[1]
    for index, ref in enumerate(refs):
        blocks = ref.at[pl.ds(0, devices - 1)]
        pltpu.make_async_copy(blocks, blocks, sems.at[first + index]).wait()


def exchange_kernel(count, *refs):
    sources, targets = refs[:count], refs[count : 2 * count]
    send_sem, recv_sem = refs[2 * count :]
    greet()
    send_all(sources, targets, send_sem, recv_sem, 0)
    wait_all(targets, recv_sem, 0)
    wait_all(sources, send_sem, 0)


def exchange(arrays, collective_id):
    count = len(arrays)
    vmem = pl.BlockSpec(memory_space=pltpu.VMEM)
    return pl.pallas_call(
        functools.partial(exchange_kernel, count),
        out_shape=tuple(jax.ShapeDtypeStruct(array.shape, array.dtype) for array in arrays),
        in_specs=[vmem] * count,
        out_specs=(vmem,) * count,
        scratch_shapes=[pltpu.SemaphoreType.DMA((count,)), pltpu.SemaphoreType.DMA((count,))],
        compiler_params=pltpu.CompilerParams(collective_id=collective_id, has_side_effects=True),
        name="exchange" + str(collective_id),
    )(*arrays)


def combined(asked, parts, cluster):
    masked = jnp.where(asked == cluster, parts, lowest)
    upper = jnp.max(jnp.max(masked, axis=0), axis=0, keepdims=True)
    total = jnp.sum(jnp.sum(jnp.exp(masked - upper[None]), axis=0), axis=0, keepdims=True)
    return upper + jnp.log(total)


def turn_kernel(column_ref, asked_ref, mass_ref, u_ref, parts_ref, outgoing_ref, send_sem, recv_sem):
    greet()
    send_all([column_ref], [parts_ref], send_sem, recv_sem, 0)
    wait_all([parts_ref], recv_sem, 0)
    asked, parts = asked_ref[...], parts_ref[...]

    outgoing = jnp.zeros(parts.shape, jnp.float32)
    for cluster in range(mass_ref.shape[0]):
        row = mass_ref[cluster : cluster + 1, :] - combined(asked, parts, cluster)
        outgoing = jnp.where(asked == cluster, row[None], outgoing)
    outgoing_ref[...] = outgoing
    send_all([outgoing_ref], [u_ref], send_sem, recv_sem, 1)
    wait_all([u_ref], recv_sem, 1)
    wait_all([column_ref, outgoing_ref], send_sem, 0)


def finish_kernel(column_ref, asked_ref, level_ref, parts_ref, send_sem, recv_sem):
    greet()
    send_all([column_ref], [parts_ref], send_sem, recv_sem, 0)
    wait_all([parts_ref], recv_sem, 0)
    asked, parts = asked_ref[...], parts_ref[...]
    for cluster in range(level_ref.shape[0]):
        level_ref[cluster : cluster + 1, :] = combined(asked, parts, cluster)
    wait_all([column_ref], send_sem, 0)


def owner_call(kernel, out, scratch, collective_id, *operands):
    vmem = pl.BlockSpec(memory_space=pltpu.VMEM)
    return pl.pallas_call(
        kernel,
        out_shape=out,
        in_specs=[vmem] * len(operands),
        out_specs=vmem,
        scratch_shapes=scratch
        + [pltpu.SemaphoreType.DMA((2,)), pltpu.SemaphoreType.DMA((2,))],
        compiler_params=pltpu.CompilerParams(collective_id=collective_id, has_side_effects=True),
        name="owner" + str(collective_id),
    )(*operands)


def bias_rows(row, ones_first):
    high = row.astype(jnp.bfloat16).astype(jnp.float32)
    rest = row - high
    middle = rest.astype(jnp.bfloat16).astype(jnp.float32)
    low = rest - middle
    index = lax.broadcasted_iota(jnp.int32, (EXTRA, row.shape[1]), 0)
    where, other = (3, 0) if ones_first else (0, 3)
    ones = jnp.where((index >= other) & (index < other + 3), 1.0, 0.0)
    return jnp.where(
        index == where,
        high,
        jnp.where(index == where + 1, middle, jnp.where(index == where + 2, low, ones)),
    )


def split_rows(row):
    high = row.astype(jnp.bfloat16).astype(jnp.float32)
    index = lax.broadcasted_iota(jnp.int32, (16, row.shape[1]), 0)
    return jnp.where(index == 0, high, jnp.where(index == 1, row - high, 0.0)).astype(jnp.bfloat16)


def whole_max(array):
    return jnp.max(jnp.max(array, axis=0, keepdims=True), axis=1, keepdims=True)


def halves():
    me, devices, columns = place()
    half = devices // 2
    side = lax.div(me, half)
    return side, me - side * half, half, columns


def wrapped(value, size):
    return value - jnp.where(value >= size, size, 0)


def spot(other, step):
    side, mine, half, columns = halves()
    near = wrapped(mine + step, half)
    base = (1 - side) * half if other else side * half
    return near, base + near


def start_copy(source, target, sems, index, where, arrival=None):
    pltpu.make_async_remote_copy(
        src_ref=source,
        dst_ref=target,
        send_sem=sems[0].at[index],
        recv_sem=sems[1].at[index if arrival is None else arrival],
        device_id=where,
        device_id_type=LOGICAL,
    ).start()


def wait_blocks(ref, count, sem):
    blocks = ref if count is None else ref.at[pl.ds(0, count)]
    pltpu.make_async_copy(blocks, blocks, sem).wait()


def plan_kernel(
    support_in, source_in, target_in, mass_in, target_mass_in, coarse_in,
    f_ref, g_ref, flag_ref,
    support_ref, names_ref, source_ref, target_ref, mass_ref, target_mass_ref, coarse_ref, input_sem,
    codes, codes_scalar, asked_near, asked_far, asked_scalar, slots_ref,
    near, mate_near, tile_out, tiles,
    beta_out, mate_beta_out, betas, mate_betas, beta_next_out, beta_next,
    columns, parts, columns_next, parts_next,
    asked, requests, owners_of,
    left, weight, sums, level_f, peaks, lifted, hot, rows,
    local_sem, send_sem, recv_sem, near_sem, mate_sem, *more,
):
    _, devices, _ = place()
    side, mine, half, _ = halves()
    inputs = (support_in, support_in, source_in, target_in, mass_in, target_mass_in, coarse_in)
    landings = (support_ref, names_ref, source_ref, target_ref, mass_ref, target_mass_ref, coarse_ref)
    clusters, features, points = source_ref.shape
    entries = support_ref.shape[1]
    slots = devices * CAP
    sems = (send_sem, recv_sem)
    mates, mate_outs, mate_tiles, stores = more[:CHUNKS], more[CHUNKS : 2 * CHUNKS], more[2 * CHUNKS : 3 * CHUNKS], more[3 * CHUNKS :]
    roomy = len(stores) == 3
    barrier = pltpu.get_barrier_semaphore()

    def each_peer(use, between=None):
        for other in range(2):
            if other and between is not None:
                between()

            def one(step, carry):
                use(other, *spot(other, step))
                return carry

            lax.fori_loop(1 - other, half, one, 0, unroll=8 if other else 5)

    each_peer(
        lambda other, near, where: pl.semaphore_signal(barrier, inc=1, device_id=where, device_id_type=LOGICAL)
    )
    loads = [
        pltpu.make_async_copy(origin, landing, input_sem.at[index])
        for index, (origin, landing) in enumerate(zip(inputs, landings))
    ]
    for load in loads:
        load.start()
    for load in loads:
        load.wait()

    block = lax.broadcasted_iota(jnp.int32, (devices, entries), 0)
    far = jnp.where(block >= half, 1, 0)
    owner_of_block = jnp.where(far == 1, 1 - side, side) * half + block - far * half
    first = jnp.full((devices, entries), clusters, jnp.int32)
    second = jnp.full((devices, entries), -1, jnp.int32)
    for cluster in range(clusters):
        name = names_ref[cluster : cluster + 1, :]
        within = name - owner_of_block * clusters
        named = (within >= 0) & (within < clusters)
        first = jnp.minimum(first, jnp.where(named, within, clusters))
        second = jnp.maximum(second, jnp.where(named, within, -1))
    first = jnp.min(first, axis=1, keepdims=True)
    second = jnp.max(second, axis=1, keepdims=True)
    own = jnp.broadcast_to(first * clusters + second, (devices, points))
    swapped = jnp.concatenate([own[half:], own[:half]], axis=0)
    lane = lax.broadcasted_iota(jnp.int32, (devices, points), 1)
    codes[...] = jnp.where(lane < points // 2, own, swapped).reshape(devices, 1, points)
    slot_block = lax.broadcasted_iota(jnp.int32, (slots, entries), 0)
    pair_first = jnp.broadcast_to(first.reshape(devices, 1, 1), (devices, CAP, entries)).reshape(slots, entries)
    pair_second = jnp.broadcast_to(second.reshape(devices, 1, 1), (devices, CAP, entries)).reshape(slots, entries)
    slot_device = lax.div(slot_block, CAP)
    slot_far = jnp.where(slot_device >= half, 1, 0)
    slot_owner = jnp.where(slot_far == 1, 1 - side, side) * half + slot_device - slot_far * half
    slot_name = slot_owner * clusters + jnp.where(lax.rem(slot_block, CAP) == 0, pair_first, pair_second)
    near[...] = 2.0 * coarse_ref[...] + target_mass_ref[...]
    pl.semaphore_wait(barrier, devices - 1)

    def ask(other, near_index, where):
        start_copy(
            codes.at[other * half + near_index], (asked_far if other else asked_near).at[mine], sems, other, where
        )

    chunk = features // CHUNKS

    def relay():
        where = spot(1, 0)[1]
        start_copy(near, mate_near, sems, 3, where)
        for index in range(CHUNKS):
            start_copy(target_ref.at[:, pl.ds(index * chunk, chunk)], mates[index], sems, RELAY + index, where)

    each_peer(ask, relay)
    local = pltpu.make_async_copy(codes, codes_scalar, local_sem.at[0])
    local.start()

    def prepare_source(cluster, carry):
        wide = source_ref[cluster].astype(jnp.float32)
        square = jnp.sum(wide * wide, axis=0, keepdims=True)
        stacked = jnp.concatenate([4.0 * wide, bias_rows(LIFT - 2.0 * square, False)], axis=0)
        left[pl.ds(cluster * points, points), :] = stacked.T.astype(jnp.bfloat16)
        return carry

    lax.fori_loop(0, clusters, prepare_source, 0, unroll=2)
    local.wait()
    asked_near[mine] = codes[mine]
    wait_blocks(asked_near, half - 1, recv_sem.at[0])
    scalars = pltpu.make_async_copy(asked_near, asked_scalar, local_sem.at[1])
    scalars.start()
    scalars.wait()

    def picks(index, lane):
        code = asked_scalar[index, 0, lane]
        chosen = lax.div(code, clusters)
        return enumerate((chosen, code - chosen * clusters))

    def member(which, offset):
        quarter = half // 2
        group = lax.div(mine, quarter)
        base = (1 - group) * quarter if which else group * quarter
        return base + wrapped(mine - group * quarter + offset, quarter)

    def serve(origin, outgoing, incoming, lane, index, arrival, shift):
        for entry, pick in picks(mine, lane):
            outgoing[mine, entry] = origin[pick]
        pltpu.make_async_copy(outgoing.at[mine], incoming.at[mine], arrival.at[shift + mine]).start()
        for which in (1, 0):

            def one(step, carry):
                near_index = member(which, step)
                for entry, pick in picks(near_index, lane):
                    outgoing[near_index, entry] = origin[pick]
                start_copy(
                    outgoing.at[near_index],
                    incoming.at[mine],
                    (send_sem, arrival),
                    index,
                    side * half + near_index,
                    shift + mine,
                )
                return carry

            lax.fori_loop(1 - which, half // 2, one, 0)

    def serve_row(origin, outgoing, incoming, lane, index):
        def one(step, carry):
            near_index, where = spot(0, step)
            for entry, pick in picks(near_index, lane):
                outgoing[near_index, pl.ds(entry, 1), :] = origin[pl.ds(pick, 1), :]
            start_copy(outgoing.at[near_index], incoming.at[mine], sems, index, where)
            return carry

        lax.fori_loop(1, half, one, 0)
        for entry, pick in picks(mine, lane):
            incoming[mine, pl.ds(entry, 1), :] = origin[pl.ds(pick, 1), :]

    wait_blocks(mate_near, None, recv_sem.at[3])
    serve_row(near, beta_out, betas, 0, 5)
    serve_row(mate_near, mate_beta_out, mate_betas, points // 2, 7)
    serve(target_ref, tile_out, tiles, 0, 4, near_sem, 0)

    def place_slots(cluster, carry):
        for entry in range(entries):
            name = support_ref[cluster, entry]
            owner = lax.div(name, clusters)
            owner_side = lax.div(owner, half)
            to = lax.rem(owner_side + side, 2) * half + owner - owner_side * half
            late = name - owner * clusters > lax.div(codes_scalar[to, 0, 0], clusters)
            slots_ref[cluster, entry] = to * CAP + late.astype(jnp.int32)
        return carry

    lax.fori_loop(0, clusters, place_slots, 0)
    for cluster in range(clusters):
        hot[:, cluster * entries : (cluster + 1) * entries] = jnp.where(
            names_ref[cluster : cluster + 1, :] == slot_name, 1.0, 0.0
        )
    def set_weights(values):
        top = whole_max(values)
        weight[...] = jnp.exp(values - top)
        return top

    def joined(sources, owner, entry):
        return jnp.concatenate([source[owner, entry] for source in sources], axis=0)

    def augmented(tile):
        wide = tile.astype(jnp.float32)
        square = jnp.sum(wide * wide, axis=0, keepdims=True)
        extra = bias_rows(LIFT - 2.0 * square, True).astype(jnp.bfloat16)
        return jnp.concatenate([tile, extra], axis=0)

    def arrivals(sources, arrival, use, begin, end):
        for which in range(2):

            def one(step, carry):
                owners = []
                for lane in range(TOGETHER):
                    owner = member(which, half // 2 - (step * TOGETHER + lane))
                    for index, source in enumerate(sources):
                        wait_blocks(source.at[owner], None, arrival.at[index * half + owner])
                    owners.append(owner)
                use(owners)
                return carry

            steps = half // 2 // TOGETHER
            lax.fori_loop(
                max(begin - which * steps, 0), max(min(end - which * steps, steps), 0), one, 0
            )

    def serve_mates(index):
        wait_blocks(mates[index], None, recv_sem.at[RELAY + index])
        serve(
            mates[index], mate_outs[index], mate_tiles[index], points // 2, PASS + index, mate_sem, index * half
        )

    def set_asked():
        wait_blocks(asked_far, half, recv_sem.at[1])
        asked_own = jnp.concatenate([asked_near[...], asked_far[...]], axis=0)[:, :, 0:1]
        asked_code = jnp.broadcast_to(asked_own, (devices, CAP, points))
        asked_first = lax.div(asked_code, clusters)
        picked = jnp.where(
            lax.broadcasted_iota(jnp.int32, (devices, CAP, points), 1) == 0,
            asked_first,
            asked_code - asked_first * clusters,
        ).reshape(slots, points)
        asked[...] = picked
        matrix = jnp.where(picked == lax.broadcasted_iota(jnp.int32, (slots, points), 1), 1.0, 0.0)
        requests[...] = matrix.astype(jnp.bfloat16)
        owners_of[...] = matrix.T[:clusters].astype(jnp.bfloat16)

    def spread(values, count):
        padded = jnp.concatenate([values, jnp.zeros((points - clusters, points), jnp.float32)], axis=0)
        total = jnp.zeros((slots, points), jnp.float32)
        for _ in range(count):
            piece = padded.astype(jnp.bfloat16)
            total = total + jnp.dot(requests[...], piece, preferred_element_type=jnp.float32)
            padded = padded - piece.astype(jnp.float32)
        return total

    def owned_levels(parts_ref):
        values = parts_ref[...].reshape(slots, points)
        names = asked[...]
        peak = jnp.concatenate(
            [
                jnp.max(jnp.where(names == cluster, values, lowest), axis=0, keepdims=True)
                for cluster in range(clusters)
            ],
            axis=0,
        )
        peak = peak.astype(jnp.bfloat16).astype(jnp.float32)
        shares = jnp.exp(values - spread(peak, 1))
        total = jnp.zeros((clusters, points), jnp.float32)
        for _ in range(2):
            piece = shares.astype(jnp.bfloat16)
            total = total + jnp.dot(owners_of[...], piece, preferred_element_type=jnp.float32)
            shares = shares - piece.astype(jnp.float32)
        return peak + jnp.log(total)

    groups = half // TOGETHER
    early = groups * EARLY // 8
    for index in range(CHUNKS - 1):
        serve_mates(index)
    wait_blocks(betas, half - 1, recv_sem.at[5])
    wait_blocks(mate_betas, half - 1, recv_sem.at[7])
    start = jnp.concatenate([betas[...], mate_betas[...]], axis=0).reshape(slots, points)
    start_top = set_weights(start)

    if roomy:
        store, gathered, total_store = stores
        span = clusters // 4
        for cluster in range(clusters):
            count = jnp.sum(hot[:, cluster * entries : (cluster + 1) * entries], axis=1, keepdims=True)
            gathered[cluster] = weight[...] * count
        total_store[...] = jnp.zeros(total_store.shape, jnp.float32)

        def use_tile(sources, offset):
            def use(owners):
                picked = [(owner, entry) for owner in owners for entry in range(CAP)]
                rhs = jnp.concatenate([augmented(joined(sources, owner, entry)) for owner, entry in picked], axis=1)
                for part in range(4):
                    first_row = part * span * points
                    values = jnp.exp(
                        jnp.dot(
                            left[first_row : first_row + span * points, :], rhs, preferred_element_type=jnp.float32
                        )
                    )
                    for lane, (owner, entry) in enumerate(picked):
                        slot = (offset + owner) * CAP + entry
                        store[slot, first_row : first_row + span * points, :] = values[
                            :, lane * points : (lane + 1) * points
                        ].astype(jnp.bfloat16)
                    for index in range(span):
                        cluster = part * span + index
                        added = 0.0
                        for lane, (owner, entry) in enumerate(picked):
                            block = values[index * points : (index + 1) * points, lane * points : (lane + 1) * points]
                            slot = (offset + owner) * CAP + entry
                            added = added + block * gathered[cluster, pl.ds(slot, 1), :]
                        total_store[cluster] += added

            return use

    else:
        right, store_even, store_odd = stores[:3]

        def use_tile(sources, offset):
            def use(owners):
                for owner in owners:
                    for entry in range(CAP):
                        right[(offset + owner) * CAP + entry] = augmented(joined(sources, owner, entry))

            return use

    arrivals([tiles], near_sem, use_tile([tiles], 0), 0, early)
    serve_mates(CHUNKS - 1)
    arrivals([tiles], near_sem, use_tile([tiles], 0), early, groups)
    set_asked()
    arrivals(mate_tiles, mate_sem, use_tile(mate_tiles, half), 0, groups)
    def close(cluster, total, top):
        row = jnp.sum(total.T, axis=0, keepdims=True)
        level = jnp.log(row) + (top - 2.0 * LIFT)
        alpha = mass_ref[pl.ds(cluster, 1), :] - level
        peak = jnp.max(alpha, axis=1, keepdims=True)
        sums[pl.ds(cluster, 1), :] = row
        level_f[pl.ds(cluster, 1), :] = level
        peaks[pl.ds(cluster, 1), :] = jnp.broadcast_to(peak, (1, points))
        lifted[cluster] = split_rows(jnp.exp(alpha - peak))

    def blocks(cluster, held, pair):
        if roomy:
            return [
                held[0][slots_ref[cluster, 2 * pair + lane], pl.ds(cluster * points, points), :] for lane in range(2)
            ]
        pairs = held[0][held[1], :, pl.ds(pair * 2 * points, 2 * points)]
        return [pairs[:, lane * points : (lane + 1) * points] for lane in range(2)]

    def build(cluster, held, pair, total):
        chosen = [slots_ref[cluster, 2 * pair + lane] for lane in range(2)]
        rhs = jnp.concatenate([right[slot] for slot in chosen], axis=1)
        values = jnp.exp(
            jnp.dot(left[pl.ds(cluster * points, points), :], rhs, preferred_element_type=jnp.float32)
        )
        held[0][held[1], :, pl.ds(pair * 2 * points, 2 * points)] = values.astype(jnp.bfloat16)
        for lane, slot in enumerate(chosen):
            total = total + values[:, lane * points : (lane + 1) * points] * weight[pl.ds(slot, 1), :]
        return total

    def forward(cluster, held, pair, total):
        for lane, values in enumerate(blocks(cluster, held, pair)):
            slot = slots_ref[cluster, 2 * pair + lane]
            total = total + values.astype(jnp.float32) * weight[pl.ds(slot, 1), :]
        return total

    def backward(cluster, held, pair):
        products = jnp.dot(
            lifted[cluster],
            jnp.concatenate(blocks(cluster, held, pair), axis=1),
            preferred_element_type=jnp.float32,
        )
        row = products[0:1] + products[1:2]
        for lane in range(2):
            rows[pl.ds(cluster * entries + 2 * pair + lane, 1), :] = row[:, lane * points : (lane + 1) * points]

    def even(index):
        return (store,) if roomy else (store_even, index)

    def odd(index):
        return (store,) if roomy else (store_odd, index)

    def sweep(make, top):
        def mixed(cluster, held, before, held_before):
            total = jnp.zeros((points, points), jnp.float32)
            for pair in range(entries // 2):
                if before is not None:
                    backward(before, held_before, pair)
                if cluster is not None:
                    total = make(cluster, held, pair, total)
            if cluster is not None:
                close(cluster, total, top)

        def both(index, carry):
            mixed(2 * index + 1, odd(index), 2 * index, even(index))
            mixed(2 * index + 2, even(index + 1), 2 * index + 1, odd(index))
            return carry

        last = clusters // 2 - 1
        mixed(0, even(0), None, None)
        lax.fori_loop(0, last, both, 0)
        mixed(clusters - 1, odd(last), clusters - 2, even(last))
        mixed(None, None, clusters - 1, odd(last))
        return finish()

    def first_sweep(top):
        def closing(cluster, carry):
            close(cluster, total_store[cluster], top)
            return carry

        def returning(index, carry):
            for lane in range(2):
                for pair in range(entries // 2):
                    backward(2 * index + lane, (store,), pair)
            return carry

        lax.fori_loop(0, clusters, closing, 0, unroll=4)
        lax.fori_loop(0, clusters // 2, returning, 0)
        return finish()

    def finish():
        peak = whole_max(peaks[...])
        scale = jnp.exp(peaks[...] - peak)
        total = jnp.zeros((slots, points), jnp.float32)
        values = jnp.concatenate(
            [
                rows[pl.ds(cluster * entries, entries), :] * scale[cluster : cluster + 1, :]
                for cluster in range(clusters)
            ],
            axis=0,
        )
        choice = hot[...].astype(jnp.bfloat16)
        for _ in range(2):
            piece = values.astype(jnp.bfloat16)
            total = total + jnp.dot(choice, piece, preferred_element_type=jnp.float32)
            values = values - piece.astype(jnp.float32)
        low = jnp.maximum(
            whole_max(jnp.where(sums[...] >= FLOOR, 0.0, 1.0)), whole_max(jnp.where(total >= FLOOR, 0.0, 1.0))
        )
        column = jnp.log(total) + (peak - 2.0 * LIFT)
        return jnp.where(low > 0.0, ALARM, column).reshape(devices, CAP, points)

    def return_columns(source, target, index):
        each_peer(
            lambda other, near_index, where: start_copy(
                source.at[other * half + near_index], target.at[other * half + mine], sems, index, where
            )
        )
        target[mine] = source[mine]
        wait_blocks(target, devices - 1, recv_sem.at[index])

    columns[...] = first_sweep(start_top) if roomy else sweep(build, start_top)
    return_columns(columns, parts, 8)
    beta_next_out[...] = spread(target_mass_ref[...] - owned_levels(parts), 3).reshape(devices, CAP, points)
    return_columns(beta_next_out, beta_next, 9)
    columns_next[...] = sweep(forward, set_weights(beta_next[...].reshape(slots, points)))
    f_ref[...] = level_f[...]
    return_columns(columns_next, parts_next, 10)
    g_ref[...] = owned_levels(parts_next)
    alarm = jnp.maximum(parts[...].reshape(slots, points), parts_next[...].reshape(slots, points))
    flag_ref[0, 0] = jnp.max(jnp.where(alarm < 1e30, 0.0, 1.0)).astype(jnp.int32)
    wait_blocks(codes, half - 1, send_sem.at[0])
    wait_blocks(codes, half, send_sem.at[1])
    for index in range(CHUNKS):
        wait_blocks(mates[index], None, send_sem.at[RELAY + index])
        wait_blocks(mate_outs[index], half - 1, send_sem.at[PASS + index])
    wait_blocks(near, None, send_sem.at[3])
    wait_blocks(tile_out, half - 1, send_sem.at[4])
    wait_blocks(beta_out, half - 1, send_sem.at[5])
    wait_blocks(mate_beta_out, half - 1, send_sem.at[7])
    wait_blocks(columns, devices - 1, send_sem.at[8])
    wait_blocks(beta_next_out, devices - 1, send_sem.at[9])
    wait_blocks(columns_next, devices - 1, send_sem.at[10])


def plan_call(support, source, target, mass, target_mass, coarse):
    devices = lax.axis_size(AXES)
    clusters, features, points = source.shape
    entries = support.shape[1]
    slots = devices * CAP
    half = devices // 2
    depth = features + EXTRA
    vmem = pl.BlockSpec(memory_space=pltpu.VMEM)
    level = jax.ShapeDtypeStruct((clusters, points), jnp.float32)
    levels = pltpu.VMEM((clusters, points), jnp.float32)
    row_block = pltpu.VMEM((devices, CAP, points), jnp.float32)
    half_row = pltpu.VMEM((half, CAP, points), jnp.float32)
    half_tile = pltpu.VMEM((half, CAP, features, points), jnp.bfloat16)
    whole_tile = pltpu.VMEM((clusters, features, points), jnp.bfloat16)
    half_code = pltpu.VMEM((half, 1, points), jnp.int32)
    roomy = slots * clusters * points * points <= ROOM
    if roomy:
        stores = [
            pltpu.VMEM((slots, clusters * points, points), jnp.bfloat16),
            pltpu.VMEM((clusters, slots, points), jnp.float32),
            pltpu.VMEM((clusters, points, points), jnp.float32),
        ]
    else:
        kernel_block = pltpu.VMEM((clusters // 2, points, entries * points), jnp.bfloat16)
        stores = [pltpu.VMEM((slots, depth, points), jnp.bfloat16), kernel_block, kernel_block, pltpu.SMEM((1,), jnp.int32)]
    sems = pltpu.SemaphoreType.DMA((PASS + CHUNKS,))
    return pl.pallas_call(
        plan_kernel,
        out_shape=(level, level, jax.ShapeDtypeStruct((1, 1), jnp.int32)),
        in_specs=[pl.BlockSpec(memory_space=pltpu.HBM)] * 6,
        out_specs=(vmem, vmem, pl.BlockSpec(memory_space=pltpu.SMEM)),
        scratch_shapes=[
            pltpu.SMEM((clusters, entries), jnp.int32),
            pltpu.VMEM((clusters, entries), jnp.int32),
            whole_tile,
            whole_tile,
            levels, levels, levels,
            pltpu.SemaphoreType.DMA((7,)),
            pltpu.VMEM((devices, 1, points), jnp.int32),
            pltpu.SMEM((devices, 1, points), jnp.int32),
            half_code,
            half_code,
            pltpu.SMEM((half, 1, points), jnp.int32),
            pltpu.SMEM((clusters, entries), jnp.int32),
            levels,
            levels,
            half_tile, half_tile,
            half_row, half_row, half_row, half_row,
            row_block, row_block, row_block, row_block, row_block, row_block,
            pltpu.VMEM((slots, points), jnp.int32),
            pltpu.VMEM((slots, points), jnp.bfloat16),
            pltpu.VMEM((clusters, slots), jnp.bfloat16),
            pltpu.VMEM((clusters * points, depth), jnp.bfloat16),
            pltpu.VMEM((slots, points), jnp.float32),
            levels, levels, levels,
            pltpu.VMEM((clusters, 16, points), jnp.bfloat16),
            pltpu.VMEM((slots, clusters * entries), jnp.float32),
            pltpu.VMEM((clusters * entries, points), jnp.float32),
            pltpu.SemaphoreType.DMA((2,)), sems, sems,
            pltpu.SemaphoreType.DMA((half,)), pltpu.SemaphoreType.DMA((CHUNKS * half,)),
        ]
        + [pltpu.VMEM((clusters, features // CHUNKS, points), jnp.bfloat16)] * CHUNKS
        + [pltpu.VMEM((half, CAP, features // CHUNKS, points), jnp.bfloat16)] * (2 * CHUNKS)
        + stores,
        compiler_params=pltpu.CompilerParams(
            collective_id=8, has_side_effects=True, vmem_limit_bytes=60 * 1024 * 1024
        ),
        name="plan",
    )(support, source, target, mass, target_mass, coarse)


def careful(source_points, target_points, source_mass, target_mass, support, coarse_potential):
    devices = lax.axis_size(AXES)
    local_count, features, points = source_points.shape
    owner = support // local_count
    within = support % local_count
    flat_owner, flat_within = owner.reshape(-1), within.reshape(-1)
    named = flat_owner[None, :] == jnp.arange(devices, dtype=jnp.int32)[:, None]
    first = jnp.min(jnp.where(named, flat_within[None, :], local_count), axis=1)
    second = jnp.max(jnp.where(named, flat_within[None, :], -1), axis=1)
    request = jnp.stack([first, second], axis=1).astype(jnp.int32)
    shape = (devices, CAP, points)
    (asked,) = exchange([jnp.broadcast_to(request[:, :, None], shape)], 0)
    first_of = jnp.sum(jnp.where(named, first[:, None], 0), axis=0).reshape(owner.shape)
    slot_list = (owner * CAP + (within > first_of).astype(jnp.int32)).astype(jnp.int32)

    target_sq = squares(target_points)
    source_sq = squares(source_points)
    u = 2.0 * (coarse_potential - target_sq) + target_mass
    matches = asked[:, :, None, :] == jnp.arange(local_count, dtype=jnp.int32)[:, None]
    sending = jnp.sum(jnp.where(matches, u, 0.0), axis=2)
    tiles, received = exchange([target_points[asked[:, :, 0]], sending], 1)
    tiles = tiles.reshape(devices * CAP, features, points)
    row_shape = jax.ShapeDtypeStruct(shape, jnp.float32)
    level_shape = jax.ShapeDtypeStruct(target_mass.shape, jnp.float32)
    buffer = pltpu.VMEM(shape, jnp.float32)
    for sweep in range(ITERS):
        level, column = sweep_call(
            slot_list, source_points, source_mass, tiles, received.reshape(devices * CAP, points)
        )
        column = column.reshape(shape)
        if sweep < ITERS - 1:
            received = owner_call(
                turn_kernel, row_shape, [buffer, buffer], 2 + sweep, column, asked, target_mass
            )
    column_level = owner_call(finish_kernel, level_shape, [buffer], 1 + ITERS, column, asked)
    return level - 2.0 * source_sq, column_level - 2.0 * target_sq


def body(source_points, target_points, source_mass, target_mass, support, coarse_potential):
    f, g, flag = plan_call(
        support, source_points, target_points, source_mass, target_mass, coarse_potential
    )

    def again():
        return careful(
            source_points, target_points, source_mass, target_mass, support, coarse_potential
        )

    f, g = lax.cond(flag[0, 0] > 0, again, lambda: (f, g))
    return -0.5 * f, -0.5 * g


def solution(mesh):
    placed = (
        P(AXES, None, None),
        P(AXES, None, None),
        P(AXES, None),
        P(AXES, None),
        P(AXES, None),
        P(AXES, None),
    )
    return jax.shard_map(
        body,
        mesh=mesh,
        in_specs=placed,
        out_specs=(P(AXES, None), P(AXES, None)),
        check_vma=False,
    )
```

```python
import functools

import jax
import jax.numpy as jnp
from jax import lax
from jax.experimental import pallas as pl
from jax.experimental.pallas import tpu as pltpu
from jax.sharding import PartitionSpec as P

CAP = 2
EXTRA = 16
LIFT = 20.0
FLOOR = 1e-10
ALARM = 3e38
ROOM = 17 * 1024 * 1024
TOGETHER = 2
EARLY = 3
CHUNKS = 1
PARTS = 4
RELAY = 11
PASS = RELAY + CHUNKS
LOGICAL = pl.DeviceIdType.LOGICAL
ITERS = 2
AXES = ("row", "col")
GROUP = 4
MESH = pl.DeviceIdType.MESH


epsilon = 0.5
lowest = -1e30


def squares(points):
    wide = points.astype(jnp.float32)
    return jnp.sum(wide * wide, axis=-2)


def pieces(row, depth):
    high = row.astype(jnp.bfloat16).astype(jnp.float32)
    rest = row - high
    middle = rest.astype(jnp.bfloat16).astype(jnp.float32)
    low = rest - middle
    index = lax.broadcasted_iota(jnp.int32, (depth, row.shape[1]), 0)
    return jnp.where(
        index == 0, high, jnp.where(index == 1, middle, jnp.where(index == 2, low, 0.0))
    )


def ones_rows(depth, points):
    index = lax.broadcasted_iota(jnp.int32, (depth, points), 0)
    return jnp.where(index < 3, 1.0, 0.0)


def fold(old_max, old_sum, scores):
    rows, lanes = scores.shape
    blocks = scores.reshape(rows // 8, 8, lanes)
    upper = jnp.maximum(old_max, jnp.max(blocks, axis=0))
    total = old_sum * jnp.exp(old_max - upper) + jnp.sum(jnp.exp(blocks - upper[None]), axis=0)
    return upper, total


def sweep_kernel(
    slots_ref, source_ref, mass_ref, tiles_ref, u_ref, row_ref, column_ref,
    tile_forward, tile_backward, run_max, run_sum,
):
    clusters, features, points = source_ref.shape
    slots = tiles_ref.shape[0]
    entries = slots_ref.shape[1]
    spare = tile_forward.shape[2] - features
    ones = ones_rows(spare, points)

    def prepare(slot, carry):
        tile = tiles_ref[slot].astype(jnp.float32)
        extra = pieces(u_ref[pl.ds(slot, 1), :], spare)
        tile_forward[slot] = jnp.concatenate([4.0 * tile, extra], axis=0).T.astype(jnp.bfloat16)
        tile_backward[slot] = jnp.concatenate([tile, ones], axis=0).astype(jnp.bfloat16)
        run_max[slot] = jnp.full((8, points), lowest, jnp.float32)
        run_sum[slot] = jnp.zeros((8, points), jnp.float32)
        return carry

    lax.fori_loop(0, slots, prepare, 0, unroll=8)

    def visit(cluster, carry):
        source = source_ref[cluster].astype(jnp.float32)
        right = jnp.concatenate([source, ones], axis=0).astype(jnp.bfloat16)

        def forward(step, state):
            lhs = jnp.concatenate(
                [tile_forward[slots_ref[cluster, step * GROUP + lane]] for lane in range(GROUP)],
                axis=0,
            )
            return fold(*state, jnp.dot(lhs, right, preferred_element_type=jnp.float32))

        start = (
            jnp.full((8, points), lowest, jnp.float32),
            jnp.zeros((8, points), jnp.float32),
        )
        upper, total = lax.fori_loop(0, entries // GROUP, forward, start, unroll=True)
        peak = jnp.max(upper, axis=0, keepdims=True)
        total = jnp.sum(total * jnp.exp(upper - peak), axis=0, keepdims=True)
        level = peak + jnp.log(total)
        row_ref[pl.ds(cluster, 1), :] = level
        extra = pieces(mass_ref[pl.ds(cluster, 1), :] - level, spare)
        left = jnp.concatenate([4.0 * source, extra], axis=0).T.astype(jnp.bfloat16)

        def backward(step, state):
            chosen = [slots_ref[cluster, step * GROUP + lane] for lane in range(GROUP)]
            held = [(run_max[slot], run_sum[slot]) for slot in chosen]
            rhs = jnp.concatenate([tile_backward[slot] for slot in chosen], axis=1)
            scores = jnp.dot(left, rhs, preferred_element_type=jnp.float32)
            fresh = [
                fold(*held[lane], scores[:, lane * points : (lane + 1) * points])
                for lane in range(GROUP)
            ]
            for slot, (new_max, new_sum) in zip(chosen, fresh):
                run_max[slot] = new_max
                run_sum[slot] = new_sum
            return state

        lax.fori_loop(0, entries // GROUP, backward, 0, unroll=True)
        return carry

    lax.fori_loop(0, clusters, visit, 0)
    upper = run_max[...]
    peak = jnp.max(upper, axis=1, keepdims=True)
    total = jnp.sum(run_sum[...] * jnp.exp(upper - peak), axis=1)
    column_ref[...] = peak[:, 0] + jnp.log(total)


def sweep_call(slot_list, source, mass, tiles, u):
    clusters, features, points = source.shape
    slots = tiles.shape[0]
    depth = 2 * features
    vmem = pl.BlockSpec(memory_space=pltpu.VMEM)
    pairs = clusters * slot_list.shape[1]
    return pl.pallas_call(
        sweep_kernel,
        out_shape=(
            jax.ShapeDtypeStruct((clusters, points), jnp.float32),
            jax.ShapeDtypeStruct((slots, points), jnp.float32),
        ),
        in_specs=[pl.BlockSpec(memory_space=pltpu.SMEM), vmem, vmem, vmem, vmem],
        out_specs=(vmem, vmem),
        scratch_shapes=[
            pltpu.VMEM((slots, points, depth), jnp.bfloat16),
            pltpu.VMEM((slots, depth, points), jnp.bfloat16),
            pltpu.VMEM((slots, 8, points), jnp.float32),
            pltpu.VMEM((slots, 8, points), jnp.float32),
        ],
        cost_estimate=pl.CostEstimate(
            flops=4 * pairs * points * points * depth,
            transcendentals=2 * pairs * points * points,
            bytes_accessed=2 * slots * features * points,
        ),
        name="sweep",
    )(slot_list, source, mass, tiles, u)


def place():
    rows, columns = lax.axis_size("row"), lax.axis_size("col")
    return lax.axis_index("row") * columns + lax.axis_index("col"), rows * columns, columns


def peer_of(step):
    me, devices, columns = place()
    peer = lax.rem(me + step, devices)
    return peer, (lax.div(peer, columns), lax.rem(peer, columns))


def greet():
    devices = place()[1]
    barrier = pltpu.get_barrier_semaphore()

    def signal(step, carry):
        pl.semaphore_signal(barrier, inc=1, device_id=peer_of(step)[1], device_id_type=MESH)
        return carry

    lax.fori_loop(1, devices, signal, 0, unroll=8)
    pl.semaphore_wait(barrier, devices - 1)


def send_all(sources, targets, send_sem, recv_sem, first):
    me, devices, _ = place()

    def send(step, carry):
        peer, where = peer_of(step)
        for index, (source, target) in enumerate(zip(sources, targets)):
            pltpu.make_async_remote_copy(
                src_ref=source.at[peer],
                dst_ref=target.at[me],
                send_sem=send_sem.at[first + index],
                recv_sem=recv_sem.at[first + index],
                device_id=where,
                device_id_type=MESH,
            ).start()
        return carry

    lax.fori_loop(1, devices, send, 0, unroll=8)
    for source, target in zip(sources, targets):
        target[me] = source[me]


def wait_all(refs, sems, first):
    devices = place()[1]
    for index, ref in enumerate(refs):
        blocks = ref.at[pl.ds(0, devices - 1)]
        pltpu.make_async_copy(blocks, blocks, sems.at[first + index]).wait()


def exchange_kernel(count, *refs):
    sources, targets = refs[:count], refs[count : 2 * count]
    send_sem, recv_sem = refs[2 * count :]
    greet()
    send_all(sources, targets, send_sem, recv_sem, 0)
    wait_all(targets, recv_sem, 0)
    wait_all(sources, send_sem, 0)


def exchange(arrays, collective_id):
    count = len(arrays)
    vmem = pl.BlockSpec(memory_space=pltpu.VMEM)
    return pl.pallas_call(
        functools.partial(exchange_kernel, count),
        out_shape=tuple(jax.ShapeDtypeStruct(array.shape, array.dtype) for array in arrays),
        in_specs=[vmem] * count,
        out_specs=(vmem,) * count,
        scratch_shapes=[pltpu.SemaphoreType.DMA((count,)), pltpu.SemaphoreType.DMA((count,))],
        compiler_params=pltpu.CompilerParams(collective_id=collective_id, has_side_effects=True),
        name="exchange" + str(collective_id),
    )(*arrays)


def combined(asked, parts, cluster):
    masked = jnp.where(asked == cluster, parts, lowest)
    upper = jnp.max(jnp.max(masked, axis=0), axis=0, keepdims=True)
    total = jnp.sum(jnp.sum(jnp.exp(masked - upper[None]), axis=0), axis=0, keepdims=True)
    return upper + jnp.log(total)


def turn_kernel(column_ref, asked_ref, mass_ref, u_ref, parts_ref, outgoing_ref, send_sem, recv_sem):
    greet()
    send_all([column_ref], [parts_ref], send_sem, recv_sem, 0)
    wait_all([parts_ref], recv_sem, 0)
    asked, parts = asked_ref[...], parts_ref[...]

    outgoing = jnp.zeros(parts.shape, jnp.float32)
    for cluster in range(mass_ref.shape[0]):
        row = mass_ref[cluster : cluster + 1, :] - combined(asked, parts, cluster)
        outgoing = jnp.where(asked == cluster, row[None], outgoing)
    outgoing_ref[...] = outgoing
    send_all([outgoing_ref], [u_ref], send_sem, recv_sem, 1)
    wait_all([u_ref], recv_sem, 1)
    wait_all([column_ref, outgoing_ref], send_sem, 0)


def finish_kernel(column_ref, asked_ref, level_ref, parts_ref, send_sem, recv_sem):
    greet()
    send_all([column_ref], [parts_ref], send_sem, recv_sem, 0)
    wait_all([parts_ref], recv_sem, 0)
    asked, parts = asked_ref[...], parts_ref[...]
    for cluster in range(level_ref.shape[0]):
        level_ref[cluster : cluster + 1, :] = combined(asked, parts, cluster)
    wait_all([column_ref], send_sem, 0)


def owner_call(kernel, out, scratch, collective_id, *operands):
    vmem = pl.BlockSpec(memory_space=pltpu.VMEM)
    return pl.pallas_call(
        kernel,
        out_shape=out,
        in_specs=[vmem] * len(operands),
        out_specs=vmem,
        scratch_shapes=scratch
        + [pltpu.SemaphoreType.DMA((2,)), pltpu.SemaphoreType.DMA((2,))],
        compiler_params=pltpu.CompilerParams(collective_id=collective_id, has_side_effects=True),
        name="owner" + str(collective_id),
    )(*operands)


def bias_rows(row, ones_first):
    high = row.astype(jnp.bfloat16).astype(jnp.float32)
    rest = row - high
    middle = rest.astype(jnp.bfloat16).astype(jnp.float32)
    low = rest - middle
    index = lax.broadcasted_iota(jnp.int32, (EXTRA, row.shape[1]), 0)
    where, other = (3, 0) if ones_first else (0, 3)
    ones = jnp.where((index >= other) & (index < other + 3), 1.0, 0.0)
    return jnp.where(
        index == where,
        high,
        jnp.where(index == where + 1, middle, jnp.where(index == where + 2, low, ones)),
    )


def split_rows(row):
    high = row.astype(jnp.bfloat16).astype(jnp.float32)
    index = lax.broadcasted_iota(jnp.int32, (16, row.shape[1]), 0)
    return jnp.where(index == 0, high, jnp.where(index == 1, row - high, 0.0)).astype(jnp.bfloat16)


def whole_max(array):
    return jnp.max(jnp.max(array, axis=0, keepdims=True), axis=1, keepdims=True)


def halves():
    me, devices, columns = place()
    half = devices // 2
    side = lax.div(me, half)
    return side, me - side * half, half, columns


def wrapped(value, size):
    return value - jnp.where(value >= size, size, 0)


def spot(other, step):
    side, mine, half, columns = halves()
    near = wrapped(mine + step, half)
    base = (1 - side) * half if other else side * half
    return near, base + near


def start_copy(source, target, sems, index, where, arrival=None):
    pltpu.make_async_remote_copy(
        src_ref=source,
        dst_ref=target,
        send_sem=sems[0].at[index],
        recv_sem=sems[1].at[index if arrival is None else arrival],
        device_id=where,
        device_id_type=LOGICAL,
    ).start()


def wait_blocks(ref, count, sem):
    blocks = ref if count is None else ref.at[pl.ds(0, count)]
    pltpu.make_async_copy(blocks, blocks, sem).wait()


def plan_kernel(
    support_in, source_in, target_in, mass_in, target_mass_in, coarse_in,
    f_ref, g_ref, flag_ref,
    support_ref, names_ref, source_ref, target_ref, mass_ref, target_mass_ref, coarse_ref, input_sem,
    codes, codes_scalar, asked_near, asked_far, asked_scalar, slots_ref,
    near, mate_near, tile_out, tiles,
    beta_out, mate_beta_out, betas, mate_betas, beta_next_out, beta_next,
    columns, parts, columns_next, parts_next,
    asked, requests, owners_of,
    left, weight, sums, level_f, peaks, lifted, hot, rows,
    local_sem, send_sem, recv_sem, near_sem, mate_sem, *more,
):
    _, devices, _ = place()
    side, mine, half, _ = halves()
    inputs = (support_in, support_in, source_in, target_in, mass_in, target_mass_in, coarse_in)
    landings = (support_ref, names_ref, source_ref, target_ref, mass_ref, target_mass_ref, coarse_ref)
    clusters, features, points = source_ref.shape
    entries = support_ref.shape[1]
    slots = devices * CAP
    sems = (send_sem, recv_sem)
    mates, mate_outs, mate_tiles, stores = more[:CHUNKS], more[CHUNKS : 2 * CHUNKS], more[2 * CHUNKS : 3 * CHUNKS], more[3 * CHUNKS :]
    roomy = len(stores) == 3
    barrier = pltpu.get_barrier_semaphore()

    def each_peer(use, between=None):
        for other in range(2):
            if other and between is not None:
                between()

            def one(step, carry):
                use(other, *spot(other, step))
                return carry

            lax.fori_loop(1 - other, half, one, 0, unroll=8 if other else 5)

    each_peer(
        lambda other, near, where: pl.semaphore_signal(barrier, inc=1, device_id=where, device_id_type=LOGICAL)
    )
    loads = [
        pltpu.make_async_copy(origin, landing, input_sem.at[index])
        for index, (origin, landing) in enumerate(zip(inputs, landings))
    ]
    for load in loads:
        load.start()
    for load in loads:
        load.wait()

    block = lax.broadcasted_iota(jnp.int32, (devices, entries), 0)
    far = jnp.where(block >= half, 1, 0)
    owner_of_block = jnp.where(far == 1, 1 - side, side) * half + block - far * half
    first = jnp.full((devices, entries), clusters, jnp.int32)
    second = jnp.full((devices, entries), -1, jnp.int32)
    for cluster in range(clusters):
        name = names_ref[cluster : cluster + 1, :]
        within = name - owner_of_block * clusters
        named = (within >= 0) & (within < clusters)
        first = jnp.minimum(first, jnp.where(named, within, clusters))
        second = jnp.maximum(second, jnp.where(named, within, -1))
    first = jnp.min(first, axis=1, keepdims=True)
    second = jnp.max(second, axis=1, keepdims=True)
    own = jnp.broadcast_to(first * clusters + second, (devices, points))
    swapped = jnp.concatenate([own[half:], own[:half]], axis=0)
    lane = lax.broadcasted_iota(jnp.int32, (devices, points), 1)
    codes[...] = jnp.where(lane < points // 2, own, swapped).reshape(devices, 1, points)
    slot_block = lax.broadcasted_iota(jnp.int32, (slots, entries), 0)
    pair_first = jnp.broadcast_to(first.reshape(devices, 1, 1), (devices, CAP, entries)).reshape(slots, entries)
    pair_second = jnp.broadcast_to(second.reshape(devices, 1, 1), (devices, CAP, entries)).reshape(slots, entries)
    slot_device = lax.div(slot_block, CAP)
    slot_far = jnp.where(slot_device >= half, 1, 0)
    slot_owner = jnp.where(slot_far == 1, 1 - side, side) * half + slot_device - slot_far * half
    slot_name = slot_owner * clusters + jnp.where(lax.rem(slot_block, CAP) == 0, pair_first, pair_second)
    near[...] = 2.0 * coarse_ref[...] + target_mass_ref[...]
    pl.semaphore_wait(barrier, devices - 1)

    def ask(other, near_index, where):
        start_copy(
            codes.at[other * half + near_index], (asked_far if other else asked_near).at[mine], sems, other, where
        )

    chunk = features // CHUNKS

    def relay():
        where = spot(1, 0)[1]
        start_copy(near, mate_near, sems, 3, where)
        for index in range(CHUNKS):
            start_copy(target_ref.at[:, pl.ds(index * chunk, chunk)], mates[index], sems, RELAY + index, where)

    each_peer(ask, relay)
    local = pltpu.make_async_copy(codes, codes_scalar, local_sem.at[0])
    local.start()

    def prepare_source(cluster, carry):
        wide = source_ref[cluster].astype(jnp.float32)
        square = jnp.sum(wide * wide, axis=0, keepdims=True)
        stacked = jnp.concatenate([4.0 * wide, bias_rows(LIFT - 2.0 * square, False)], axis=0)
        left[pl.ds(cluster * points, points), :] = stacked.T.astype(jnp.bfloat16)
        return carry

    lax.fori_loop(0, clusters, prepare_source, 0, unroll=2)
    local.wait()
    asked_near[mine] = codes[mine]
    wait_blocks(asked_near, half - 1, recv_sem.at[0])
    scalars = pltpu.make_async_copy(asked_near, asked_scalar, local_sem.at[1])
    scalars.start()
    scalars.wait()

    def picks(index, lane):
        code = asked_scalar[index, 0, lane]
        chosen = lax.div(code, clusters)
        return enumerate((chosen, code - chosen * clusters))

    def member(which, offset):
        quarter = half // 2
        group = lax.div(mine, quarter)
        base = (1 - group) * quarter if which else group * quarter
        return base + wrapped(mine - group * quarter + offset, quarter)

    def serve(origin, outgoing, incoming, lane, index, arrival, shift):
        for entry, pick in picks(mine, lane):
            outgoing[mine, entry] = origin[pick]
        pltpu.make_async_copy(outgoing.at[mine], incoming.at[mine], arrival.at[shift + mine]).start()
        for which in (0, 1):

            def one(step, carry):
                near_index = member(which, step)
                for entry, pick in picks(near_index, lane):
                    outgoing[near_index, entry] = origin[pick]
                start_copy(
                    outgoing.at[near_index],
                    incoming.at[mine],
                    (send_sem, arrival),
                    index,
                    side * half + near_index,
                    shift + mine,
                )
                return carry

            lax.fori_loop(1 - which, half // 2, one, 0, unroll=4 if which else half // 2 - 1)

    def serve_row(origin, outgoing, incoming, lane, index):
        def one(step, carry):
            near_index, where = spot(0, step)
            for entry, pick in picks(near_index, lane):
                outgoing[near_index, pl.ds(entry, 1), :] = origin[pl.ds(pick, 1), :]
            start_copy(outgoing.at[near_index], incoming.at[mine], sems, index, where)
            return carry

        lax.fori_loop(1, half, one, 0, unroll=5)
        for entry, pick in picks(mine, lane):
            incoming[mine, pl.ds(entry, 1), :] = origin[pl.ds(pick, 1), :]

    wait_blocks(mate_near, None, recv_sem.at[3])
    serve_row(near, beta_out, betas, 0, 5)
    serve_row(mate_near, mate_beta_out, mate_betas, points // 2, 7)
    serve(target_ref, tile_out, tiles, 0, 4, near_sem, 0)

    def place_slots(cluster, carry):
        for entry in range(entries):
            name = support_ref[cluster, entry]
            owner = lax.div(name, clusters)
            owner_side = lax.div(owner, half)
            to = lax.rem(owner_side + side, 2) * half + owner - owner_side * half
            late = name - owner * clusters > lax.div(codes_scalar[to, 0, 0], clusters)
            slots_ref[cluster, entry] = to * CAP + late.astype(jnp.int32)
        return carry

    lax.fori_loop(0, clusters, place_slots, 0)
    for cluster in range(clusters):
        hot[:, cluster * entries : (cluster + 1) * entries] = jnp.where(
            names_ref[cluster : cluster + 1, :] == slot_name, 1.0, 0.0
        )
    def set_weights(values):
        top = whole_max(values)
        weight[...] = jnp.exp(values - top)
        return top

    def joined(sources, owner, entry):
        return jnp.concatenate([source[owner, entry] for source in sources], axis=0)

    def augmented(tile):
        wide = tile.astype(jnp.float32)
        square = jnp.sum(wide * wide, axis=0, keepdims=True)
        extra = bias_rows(LIFT - 2.0 * square, True).astype(jnp.bfloat16)
        return jnp.concatenate([tile, extra], axis=0)

    def arrivals(sources, arrival, use, begin, end):
        for which in range(2):

            def one(step, carry):
                owners = []
                for lane in range(TOGETHER):
                    owner = member(which, half // 2 - (step * TOGETHER + lane))
                    for index, source in enumerate(sources):
                        wait_blocks(source.at[owner], None, arrival.at[index * half + owner])
                    owners.append(owner)
                use(owners)
                return carry

            steps = half // 2 // TOGETHER
            lax.fori_loop(
                max(begin - which * steps, 0), max(min(end - which * steps, steps), 0), one, 0
            )

    def serve_mates(index):
        wait_blocks(mates[index], None, recv_sem.at[RELAY + index])
        serve(
            mates[index], mate_outs[index], mate_tiles[index], points // 2, PASS + index, mate_sem, index * half
        )

    def set_asked():
        wait_blocks(asked_far, half, recv_sem.at[1])
        asked_own = jnp.concatenate([asked_near[...], asked_far[...]], axis=0)[:, :, 0:1]
        asked_code = jnp.broadcast_to(asked_own, (devices, CAP, points))
        asked_first = lax.div(asked_code, clusters)
        picked = jnp.where(
            lax.broadcasted_iota(jnp.int32, (devices, CAP, points), 1) == 0,
            asked_first,
            asked_code - asked_first * clusters,
        ).reshape(slots, points)
        asked[...] = picked
        matrix = jnp.where(picked == lax.broadcasted_iota(jnp.int32, (slots, points), 1), 1.0, 0.0)
        requests[...] = matrix.astype(jnp.bfloat16)
        owners_of[...] = matrix.T[:clusters].astype(jnp.bfloat16)

    def spread(values, count):
        padded = jnp.concatenate([values, jnp.zeros((points - clusters, points), jnp.float32)], axis=0)
        total = jnp.zeros((slots, points), jnp.float32)
        for _ in range(count):
            piece = padded.astype(jnp.bfloat16)
            total = total + jnp.dot(requests[...], piece, preferred_element_type=jnp.float32)
            padded = padded - piece.astype(jnp.float32)
        return total

    def owned_levels(parts_ref):
        values = parts_ref[...].reshape(slots, points)
        names = asked[...]
        peak = jnp.concatenate(
            [
                jnp.max(jnp.where(names == cluster, values, lowest), axis=0, keepdims=True)
                for cluster in range(clusters)
            ],
            axis=0,
        )
        peak = peak.astype(jnp.bfloat16).astype(jnp.float32)
        shares = jnp.exp(values - spread(peak, 1))
        total = jnp.zeros((clusters, points), jnp.float32)
        for _ in range(2):
            piece = shares.astype(jnp.bfloat16)
            total = total + jnp.dot(owners_of[...], piece, preferred_element_type=jnp.float32)
            shares = shares - piece.astype(jnp.float32)
        return peak + jnp.log(total)

    groups = half // TOGETHER
    early = groups * EARLY // 8
    for index in range(CHUNKS - 1):
        serve_mates(index)
    wait_blocks(betas, half - 1, recv_sem.at[5])
    wait_blocks(mate_betas, half - 1, recv_sem.at[7])
    start = jnp.concatenate([betas[...], mate_betas[...]], axis=0).reshape(slots, points)
    start_top = set_weights(start)

    if roomy:
        store, gathered, total_store = stores
        span = clusters // 4
        for cluster in range(clusters):
            count = jnp.sum(hot[:, cluster * entries : (cluster + 1) * entries], axis=1, keepdims=True)
            gathered[cluster] = weight[...] * count
        total_store[...] = jnp.zeros(total_store.shape, jnp.float32)

        def use_tile(sources, offset):
            def use(owners):
                picked = [(owner, entry) for owner in owners for entry in range(CAP)]
                rhs = jnp.concatenate([augmented(joined(sources, owner, entry)) for owner, entry in picked], axis=1)
                for part in range(4):
                    first_row = part * span * points
                    values = jnp.exp(
                        jnp.dot(
                            left[first_row : first_row + span * points, :], rhs, preferred_element_type=jnp.float32
                        )
                    )
                    for lane, (owner, entry) in enumerate(picked):
                        slot = (offset + owner) * CAP + entry
                        store[slot, first_row : first_row + span * points, :] = values[
                            :, lane * points : (lane + 1) * points
                        ].astype(jnp.bfloat16)
                    for index in range(span):
                        cluster = part * span + index
                        added = 0.0
                        for lane, (owner, entry) in enumerate(picked):
                            block = values[index * points : (index + 1) * points, lane * points : (lane + 1) * points]
                            slot = (offset + owner) * CAP + entry
                            added = added + block * gathered[cluster, pl.ds(slot, 1), :]
                        total_store[cluster] += added

            return use

    else:
        right, store_even, store_odd = stores[:3]

        def use_tile(sources, offset):
            def use(owners):
                for owner in owners:
                    for entry in range(CAP):
                        right[(offset + owner) * CAP + entry] = augmented(joined(sources, owner, entry))

            return use

    arrivals([tiles], near_sem, use_tile([tiles], 0), 0, early)
    serve_mates(CHUNKS - 1)
    arrivals([tiles], near_sem, use_tile([tiles], 0), early, groups)
    set_asked()
    arrivals(mate_tiles, mate_sem, use_tile(mate_tiles, half), 0, groups)
    def close(cluster, total, top):
        row = jnp.sum(total.T, axis=0, keepdims=True)
        level = jnp.log(row) + (top - 2.0 * LIFT)
        alpha = mass_ref[pl.ds(cluster, 1), :] - level
        peak = jnp.max(alpha, axis=1, keepdims=True)
        sums[pl.ds(cluster, 1), :] = row
        level_f[pl.ds(cluster, 1), :] = level
        peaks[pl.ds(cluster, 1), :] = jnp.broadcast_to(peak, (1, points))
        lifted[cluster] = split_rows(jnp.exp(alpha - peak))

    def blocks(cluster, held, pair):
        if roomy:
            return [
                held[0][slots_ref[cluster, 2 * pair + lane], pl.ds(cluster * points, points), :] for lane in range(2)
            ]
        pairs = held[0][held[1], :, pl.ds(pair * 2 * points, 2 * points)]
        return [pairs[:, lane * points : (lane + 1) * points] for lane in range(2)]

    def build(cluster, held, pair, total):
        chosen = [slots_ref[cluster, 2 * pair + lane] for lane in range(2)]
        rhs = jnp.concatenate([right[slot] for slot in chosen], axis=1)
        values = jnp.exp(
            jnp.dot(left[pl.ds(cluster * points, points), :], rhs, preferred_element_type=jnp.float32)
        )
        held[0][held[1], :, pl.ds(pair * 2 * points, 2 * points)] = values.astype(jnp.bfloat16)
        for lane, slot in enumerate(chosen):
            total = total + values[:, lane * points : (lane + 1) * points] * weight[pl.ds(slot, 1), :]
        return total

    def forward(cluster, held, pair, total):
        for lane, values in enumerate(blocks(cluster, held, pair)):
            slot = slots_ref[cluster, 2 * pair + lane]
            total = total + values.astype(jnp.float32) * weight[pl.ds(slot, 1), :]
        return total

    def backward(cluster, held, pair):
        products = jnp.dot(
            lifted[cluster],
            jnp.concatenate(blocks(cluster, held, pair), axis=1),
            preferred_element_type=jnp.float32,
        )
        row = products[0:1] + products[1:2]
        for lane in range(2):
            rows[pl.ds(cluster * entries + 2 * pair + lane, 1), :] = row[:, lane * points : (lane + 1) * points]

    def even(index):
        return (store,) if roomy else (store_even, index)

    def odd(index):
        return (store,) if roomy else (store_odd, index)

    def sweep(make, top):
        def mixed(cluster, held, before, held_before):
            total = None if cluster is None else total_store[cluster] if make is None else jnp.zeros((points, points), jnp.float32)
            done = []
            pairs = entries // 2
            for part in range(PARTS):
                for pair in range(part * pairs // PARTS, (part + 1) * pairs // PARTS):
                    if before is not None:
                        backward(before, held_before, pair)
                    if make is not None and cluster is not None:
                        total = make(cluster, held, pair, total)
            if cluster is not None:
                close(cluster, jnp.concatenate(done, axis=0) if done else total, top)

        def both(index, carry):
            mixed(2 * index + 1, odd(index), 2 * index, even(index))
            mixed(2 * index + 2, even(index + 1), 2 * index + 1, odd(index))
            return carry

        last = clusters // 2 - 1
        mixed(0, even(0), None, None)
        lax.fori_loop(0, last, both, 0)
        mixed(clusters - 1, odd(last), clusters - 2, even(last))
        mixed(None, None, clusters - 1, odd(last))
        return finish()

    def finish():
        peak = whole_max(peaks[...])
        scale = jnp.exp(peaks[...] - peak)
        total = jnp.zeros((slots, points), jnp.float32)
        values = jnp.concatenate(
            [
                rows[pl.ds(cluster * entries, entries), :] * scale[cluster : cluster + 1, :]
                for cluster in range(clusters)
            ],
            axis=0,
        )
        choice = hot[...].astype(jnp.bfloat16)
        for _ in range(2):
            piece = values.astype(jnp.bfloat16)
            total = total + jnp.dot(choice, piece, preferred_element_type=jnp.float32)
            values = values - piece.astype(jnp.float32)
        low = jnp.maximum(
            whole_max(jnp.where(sums[...] >= FLOOR, 0.0, 1.0)), whole_max(jnp.where(total >= FLOOR, 0.0, 1.0))
        )
        column = jnp.log(total) + (peak - 2.0 * LIFT)
        return jnp.where(low > 0.0, ALARM, column).reshape(devices, CAP, points)

    def return_columns(source, target, index):
        each_peer(
            lambda other, near_index, where: start_copy(
                source.at[other * half + near_index], target.at[other * half + mine], sems, index, where
            )
        )
        target[mine] = source[mine]
        wait_blocks(target, devices - 1, recv_sem.at[index])

    columns[...] = sweep(None if roomy else build, start_top)
    return_columns(columns, parts, 8)
    beta_next_out[...] = spread(target_mass_ref[...] - owned_levels(parts), 3).reshape(devices, CAP, points)
    return_columns(beta_next_out, beta_next, 9)
    columns_next[...] = sweep(forward, set_weights(beta_next[...].reshape(slots, points)))
    f_ref[...] = level_f[...]
    return_columns(columns_next, parts_next, 10)
    g_ref[...] = owned_levels(parts_next)
    alarm = jnp.maximum(parts[...].reshape(slots, points), parts_next[...].reshape(slots, points))
    flag_ref[0, 0] = jnp.max(jnp.where(alarm < 1e30, 0.0, 1.0)).astype(jnp.int32)
    wait_blocks(codes, half - 1, send_sem.at[0])
    wait_blocks(codes, half, send_sem.at[1])
    for index in range(CHUNKS):
        wait_blocks(mates[index], None, send_sem.at[RELAY + index])
        wait_blocks(mate_outs[index], half - 1, send_sem.at[PASS + index])
    wait_blocks(near, None, send_sem.at[3])
    wait_blocks(tile_out, half - 1, send_sem.at[4])
    wait_blocks(beta_out, half - 1, send_sem.at[5])
    wait_blocks(mate_beta_out, half - 1, send_sem.at[7])
    wait_blocks(columns, devices - 1, send_sem.at[8])
    wait_blocks(beta_next_out, devices - 1, send_sem.at[9])
    wait_blocks(columns_next, devices - 1, send_sem.at[10])


def plan_call(support, source, target, mass, target_mass, coarse):
    devices = lax.axis_size(AXES)
    clusters, features, points = source.shape
    entries = support.shape[1]
    slots = devices * CAP
    half = devices // 2
    depth = features + EXTRA
    vmem = pl.BlockSpec(memory_space=pltpu.VMEM)
    level = jax.ShapeDtypeStruct((clusters, points), jnp.float32)
    levels = pltpu.VMEM((clusters, points), jnp.float32)
    row_block = pltpu.VMEM((devices, CAP, points), jnp.float32)
    half_row = pltpu.VMEM((half, CAP, points), jnp.float32)
    half_tile = pltpu.VMEM((half, CAP, features, points), jnp.bfloat16)
    whole_tile = pltpu.VMEM((clusters, features, points), jnp.bfloat16)
    half_code = pltpu.VMEM((half, 1, points), jnp.int32)
    roomy = slots * clusters * points * points <= ROOM
    if roomy:
        stores = [
            pltpu.VMEM((slots, clusters * points, points), jnp.bfloat16),
            pltpu.VMEM((clusters, slots, points), jnp.float32),
            pltpu.VMEM((clusters, points, points), jnp.float32),
        ]
    else:
        kernel_block = pltpu.VMEM((clusters // 2, points, entries * points), jnp.bfloat16)
        stores = [pltpu.VMEM((slots, depth, points), jnp.bfloat16), kernel_block, kernel_block, pltpu.SMEM((1,), jnp.int32)]
    sems = pltpu.SemaphoreType.DMA((PASS + CHUNKS,))
    return pl.pallas_call(
        plan_kernel,
        out_shape=(level, level, jax.ShapeDtypeStruct((1, 1), jnp.int32)),
        in_specs=[pl.BlockSpec(memory_space=pltpu.HBM)] * 6,
        out_specs=(vmem, vmem, pl.BlockSpec(memory_space=pltpu.SMEM)),
        scratch_shapes=[
            pltpu.SMEM((clusters, entries), jnp.int32),
            pltpu.VMEM((clusters, entries), jnp.int32),
            whole_tile,
            whole_tile,
            levels, levels, levels,
            pltpu.SemaphoreType.DMA((7,)),
            pltpu.VMEM((devices, 1, points), jnp.int32),
            pltpu.SMEM((devices, 1, points), jnp.int32),
            half_code,
            half_code,
            pltpu.SMEM((half, 1, points), jnp.int32),
            pltpu.SMEM((clusters, entries), jnp.int32),
            levels,
            levels,
            half_tile, half_tile,
            half_row, half_row, half_row, half_row,
            row_block, row_block, row_block, row_block, row_block, row_block,
            pltpu.VMEM((slots, points), jnp.int32),
            pltpu.VMEM((slots, points), jnp.bfloat16),
            pltpu.VMEM((clusters, slots), jnp.bfloat16),
            pltpu.VMEM((clusters * points, depth), jnp.bfloat16),
            pltpu.VMEM((slots, points), jnp.float32),
            levels, levels, levels,
            pltpu.VMEM((clusters, 16, points), jnp.bfloat16),
            pltpu.VMEM((slots, clusters * entries), jnp.float32),
            pltpu.VMEM((clusters * entries, points), jnp.float32),
            pltpu.SemaphoreType.DMA((2,)), sems, sems,
            pltpu.SemaphoreType.DMA((half,)), pltpu.SemaphoreType.DMA((CHUNKS * half,)),
        ]
        + [pltpu.VMEM((clusters, features // CHUNKS, points), jnp.bfloat16)] * CHUNKS
        + [pltpu.VMEM((half, CAP, features // CHUNKS, points), jnp.bfloat16)] * (2 * CHUNKS)
        + stores,
        compiler_params=pltpu.CompilerParams(
            collective_id=8, has_side_effects=True, vmem_limit_bytes=60 * 1024 * 1024
        ),
        name="plan",
    )(support, source, target, mass, target_mass, coarse)


def careful(source_points, target_points, source_mass, target_mass, support, coarse_potential):
    devices = lax.axis_size(AXES)
    local_count, features, points = source_points.shape
    owner = support // local_count
    within = support % local_count
    flat_owner, flat_within = owner.reshape(-1), within.reshape(-1)
    named = flat_owner[None, :] == jnp.arange(devices, dtype=jnp.int32)[:, None]
    first = jnp.min(jnp.where(named, flat_within[None, :], local_count), axis=1)
    second = jnp.max(jnp.where(named, flat_within[None, :], -1), axis=1)
    request = jnp.stack([first, second], axis=1).astype(jnp.int32)
    shape = (devices, CAP, points)
    (asked,) = exchange([jnp.broadcast_to(request[:, :, None], shape)], 0)
    first_of = jnp.sum(jnp.where(named, first[:, None], 0), axis=0).reshape(owner.shape)
    slot_list = (owner * CAP + (within > first_of).astype(jnp.int32)).astype(jnp.int32)

    target_sq = squares(target_points)
    source_sq = squares(source_points)
    u = 2.0 * (coarse_potential - target_sq) + target_mass
    matches = asked[:, :, None, :] == jnp.arange(local_count, dtype=jnp.int32)[:, None]
    sending = jnp.sum(jnp.where(matches, u, 0.0), axis=2)
    tiles, received = exchange([target_points[asked[:, :, 0]], sending], 1)
    tiles = tiles.reshape(devices * CAP, features, points)
    row_shape = jax.ShapeDtypeStruct(shape, jnp.float32)
    level_shape = jax.ShapeDtypeStruct(target_mass.shape, jnp.float32)
    buffer = pltpu.VMEM(shape, jnp.float32)
    for sweep in range(ITERS):
        level, column = sweep_call(
            slot_list, source_points, source_mass, tiles, received.reshape(devices * CAP, points)
        )
        column = column.reshape(shape)
        if sweep < ITERS - 1:
            received = owner_call(
                turn_kernel, row_shape, [buffer, buffer], 2 + sweep, column, asked, target_mass
            )
    column_level = owner_call(finish_kernel, level_shape, [buffer], 1 + ITERS, column, asked)
    return level - 2.0 * source_sq, column_level - 2.0 * target_sq


def body(source_points, target_points, source_mass, target_mass, support, coarse_potential):
    f, g, flag = plan_call(
        support, source_points, target_points, source_mass, target_mass, coarse_potential
    )

    def again():
        return careful(
            source_points, target_points, source_mass, target_mass, support, coarse_potential
        )

    f, g = lax.cond(flag[0, 0] > 0, again, lambda: (f, g))
    return -0.5 * f, -0.5 * g


def solution(mesh):
    placed = (
        P(AXES, None, None),
        P(AXES, None, None),
        P(AXES, None),
        P(AXES, None),
        P(AXES, None),
        P(AXES, None),
    )
    return jax.shard_map(
        body,
        mesh=mesh,
        in_specs=placed,
        out_specs=(P(AXES, None), P(AXES, None)),
        check_vma=False,
    )
```

```python
import functools

import jax
import jax.numpy as jnp
from jax import lax
from jax.experimental import pallas as pl
from jax.experimental.pallas import tpu as pltpu
from jax.sharding import PartitionSpec as P

CAP = 2
EXTRA = 16
LIFT = 20.0
FLOOR = 1e-10
ALARM = 3e38
ROOM = 17 * 1024 * 1024
TOGETHER = 4
EARLY = 3
CHUNKS = 1
PARTS = 4
RELAY = 11
PASS = RELAY + CHUNKS
LOGICAL = pl.DeviceIdType.LOGICAL
ITERS = 2
AXES = ("row", "col")
GROUP = 4
MESH = pl.DeviceIdType.MESH


epsilon = 0.5
lowest = -1e30


def squares(points):
    wide = points.astype(jnp.float32)
    return jnp.sum(wide * wide, axis=-2)


def pieces(row, depth):
    high = row.astype(jnp.bfloat16).astype(jnp.float32)
    rest = row - high
    middle = rest.astype(jnp.bfloat16).astype(jnp.float32)
    low = rest - middle
    index = lax.broadcasted_iota(jnp.int32, (depth, row.shape[1]), 0)
    return jnp.where(
        index == 0, high, jnp.where(index == 1, middle, jnp.where(index == 2, low, 0.0))
    )


def ones_rows(depth, points):
    index = lax.broadcasted_iota(jnp.int32, (depth, points), 0)
    return jnp.where(index < 3, 1.0, 0.0)


def fold(old_max, old_sum, scores):
    rows, lanes = scores.shape
    blocks = scores.reshape(rows // 8, 8, lanes)
    upper = jnp.maximum(old_max, jnp.max(blocks, axis=0))
    total = old_sum * jnp.exp(old_max - upper) + jnp.sum(jnp.exp(blocks - upper[None]), axis=0)
    return upper, total


def sweep_kernel(
    slots_ref, source_ref, mass_ref, tiles_ref, u_ref, row_ref, column_ref,
    tile_forward, tile_backward, run_max, run_sum,
):
    clusters, features, points = source_ref.shape
    slots = tiles_ref.shape[0]
    entries = slots_ref.shape[1]
    spare = tile_forward.shape[2] - features
    ones = ones_rows(spare, points)

    def prepare(slot, carry):
        tile = tiles_ref[slot].astype(jnp.float32)
        extra = pieces(u_ref[pl.ds(slot, 1), :], spare)
        tile_forward[slot] = jnp.concatenate([4.0 * tile, extra], axis=0).T.astype(jnp.bfloat16)
        tile_backward[slot] = jnp.concatenate([tile, ones], axis=0).astype(jnp.bfloat16)
        run_max[slot] = jnp.full((8, points), lowest, jnp.float32)
        run_sum[slot] = jnp.zeros((8, points), jnp.float32)
        return carry

    lax.fori_loop(0, slots, prepare, 0, unroll=8)

    def visit(cluster, carry):
        source = source_ref[cluster].astype(jnp.float32)
        right = jnp.concatenate([source, ones], axis=0).astype(jnp.bfloat16)

        def forward(step, state):
            lhs = jnp.concatenate(
                [tile_forward[slots_ref[cluster, step * GROUP + lane]] for lane in range(GROUP)],
                axis=0,
            )
            return fold(*state, jnp.dot(lhs, right, preferred_element_type=jnp.float32))

        start = (
            jnp.full((8, points), lowest, jnp.float32),
            jnp.zeros((8, points), jnp.float32),
        )
        upper, total = lax.fori_loop(0, entries // GROUP, forward, start, unroll=True)
        peak = jnp.max(upper, axis=0, keepdims=True)
        total = jnp.sum(total * jnp.exp(upper - peak), axis=0, keepdims=True)
        level = peak + jnp.log(total)
        row_ref[pl.ds(cluster, 1), :] = level
        extra = pieces(mass_ref[pl.ds(cluster, 1), :] - level, spare)
        left = jnp.concatenate([4.0 * source, extra], axis=0).T.astype(jnp.bfloat16)

        def backward(step, state):
            chosen = [slots_ref[cluster, step * GROUP + lane] for lane in range(GROUP)]
            held = [(run_max[slot], run_sum[slot]) for slot in chosen]
            rhs = jnp.concatenate([tile_backward[slot] for slot in chosen], axis=1)
            scores = jnp.dot(left, rhs, preferred_element_type=jnp.float32)
            fresh = [
                fold(*held[lane], scores[:, lane * points : (lane + 1) * points])
                for lane in range(GROUP)
            ]
            for slot, (new_max, new_sum) in zip(chosen, fresh):
                run_max[slot] = new_max
                run_sum[slot] = new_sum
            return state

        lax.fori_loop(0, entries // GROUP, backward, 0, unroll=True)
        return carry

    lax.fori_loop(0, clusters, visit, 0)
    upper = run_max[...]
    peak = jnp.max(upper, axis=1, keepdims=True)
    total = jnp.sum(run_sum[...] * jnp.exp(upper - peak), axis=1)
    column_ref[...] = peak[:, 0] + jnp.log(total)


def sweep_call(slot_list, source, mass, tiles, u):
    clusters, features, points = source.shape
    slots = tiles.shape[0]
    depth = 2 * features
    vmem = pl.BlockSpec(memory_space=pltpu.VMEM)
    pairs = clusters * slot_list.shape[1]
    return pl.pallas_call(
        sweep_kernel,
        out_shape=(
            jax.ShapeDtypeStruct((clusters, points), jnp.float32),
            jax.ShapeDtypeStruct((slots, points), jnp.float32),
        ),
        in_specs=[pl.BlockSpec(memory_space=pltpu.SMEM), vmem, vmem, vmem, vmem],
        out_specs=(vmem, vmem),
        scratch_shapes=[
            pltpu.VMEM((slots, points, depth), jnp.bfloat16),
            pltpu.VMEM((slots, depth, points), jnp.bfloat16),
            pltpu.VMEM((slots, 8, points), jnp.float32),
            pltpu.VMEM((slots, 8, points), jnp.float32),
        ],
        cost_estimate=pl.CostEstimate(
            flops=4 * pairs * points * points * depth,
            transcendentals=2 * pairs * points * points,
            bytes_accessed=2 * slots * features * points,
        ),
        name="sweep",
    )(slot_list, source, mass, tiles, u)


def place():
    rows, columns = lax.axis_size("row"), lax.axis_size("col")
    return lax.axis_index("row") * columns + lax.axis_index("col"), rows * columns, columns


def peer_of(step):
    me, devices, columns = place()
    peer = lax.rem(me + step, devices)
    return peer, (lax.div(peer, columns), lax.rem(peer, columns))


def greet():
    devices = place()[1]
    barrier = pltpu.get_barrier_semaphore()

    def signal(step, carry):
        pl.semaphore_signal(barrier, inc=1, device_id=peer_of(step)[1], device_id_type=MESH)
        return carry

    lax.fori_loop(1, devices, signal, 0, unroll=8)
    pl.semaphore_wait(barrier, devices - 1)


def send_all(sources, targets, send_sem, recv_sem, first):
    me, devices, _ = place()

    def send(step, carry):
        peer, where = peer_of(step)
        for index, (source, target) in enumerate(zip(sources, targets)):
            pltpu.make_async_remote_copy(
                src_ref=source.at[peer],
                dst_ref=target.at[me],
                send_sem=send_sem.at[first + index],
                recv_sem=recv_sem.at[first + index],
                device_id=where,
                device_id_type=MESH,
            ).start()
        return carry

    lax.fori_loop(1, devices, send, 0, unroll=8)
    for source, target in zip(sources, targets):
        target[me] = source[me]


def wait_all(refs, sems, first):
    devices = place()[1]
    for index, ref in enumerate(refs):
        blocks = ref.at[pl.ds(0, devices - 1)]
        pltpu.make_async_copy(blocks, blocks, sems.at[first + index]).wait()


def exchange_kernel(count, *refs):
    sources, targets = refs[:count], refs[count : 2 * count]
    send_sem, recv_sem = refs[2 * count :]
    greet()
    send_all(sources, targets, send_sem, recv_sem, 0)
    wait_all(targets, recv_sem, 0)
    wait_all(sources, send_sem, 0)


def exchange(arrays, collective_id):
    count = len(arrays)
    vmem = pl.BlockSpec(memory_space=pltpu.VMEM)
    return pl.pallas_call(
        functools.partial(exchange_kernel, count),
        out_shape=tuple(jax.ShapeDtypeStruct(array.shape, array.dtype) for array in arrays),
        in_specs=[vmem] * count,
        out_specs=(vmem,) * count,
        scratch_shapes=[pltpu.SemaphoreType.DMA((count,)), pltpu.SemaphoreType.DMA((count,))],
        compiler_params=pltpu.CompilerParams(collective_id=collective_id, has_side_effects=True),
        name="exchange" + str(collective_id),
    )(*arrays)


def combined(asked, parts, cluster):
    masked = jnp.where(asked == cluster, parts, lowest)
    upper = jnp.max(jnp.max(masked, axis=0), axis=0, keepdims=True)
    total = jnp.sum(jnp.sum(jnp.exp(masked - upper[None]), axis=0), axis=0, keepdims=True)
    return upper + jnp.log(total)


def turn_kernel(column_ref, asked_ref, mass_ref, u_ref, parts_ref, outgoing_ref, send_sem, recv_sem):
    greet()
    send_all([column_ref], [parts_ref], send_sem, recv_sem, 0)
    wait_all([parts_ref], recv_sem, 0)
    asked, parts = asked_ref[...], parts_ref[...]

    outgoing = jnp.zeros(parts.shape, jnp.float32)
    for cluster in range(mass_ref.shape[0]):
        row = mass_ref[cluster : cluster + 1, :] - combined(asked, parts, cluster)
        outgoing = jnp.where(asked == cluster, row[None], outgoing)
    outgoing_ref[...] = outgoing
    send_all([outgoing_ref], [u_ref], send_sem, recv_sem, 1)
    wait_all([u_ref], recv_sem, 1)
    wait_all([column_ref, outgoing_ref], send_sem, 0)


def finish_kernel(column_ref, asked_ref, level_ref, parts_ref, send_sem, recv_sem):
    greet()
    send_all([column_ref], [parts_ref], send_sem, recv_sem, 0)
    wait_all([parts_ref], recv_sem, 0)
    asked, parts = asked_ref[...], parts_ref[...]
    for cluster in range(level_ref.shape[0]):
        level_ref[cluster : cluster + 1, :] = combined(asked, parts, cluster)
    wait_all([column_ref], send_sem, 0)


def owner_call(kernel, out, scratch, collective_id, *operands):
    vmem = pl.BlockSpec(memory_space=pltpu.VMEM)
    return pl.pallas_call(
        kernel,
        out_shape=out,
        in_specs=[vmem] * len(operands),
        out_specs=vmem,
        scratch_shapes=scratch
        + [pltpu.SemaphoreType.DMA((2,)), pltpu.SemaphoreType.DMA((2,))],
        compiler_params=pltpu.CompilerParams(collective_id=collective_id, has_side_effects=True),
        name="owner" + str(collective_id),
    )(*operands)


def bias_rows(row, ones_first):
    high = row.astype(jnp.bfloat16).astype(jnp.float32)
    rest = row - high
    middle = rest.astype(jnp.bfloat16).astype(jnp.float32)
    low = rest - middle
    index = lax.broadcasted_iota(jnp.int32, (EXTRA, row.shape[1]), 0)
    where, other = (3, 0) if ones_first else (0, 3)
    ones = jnp.where((index >= other) & (index < other + 3), 1.0, 0.0)
    return jnp.where(
        index == where,
        high,
        jnp.where(index == where + 1, middle, jnp.where(index == where + 2, low, ones)),
    )


def split_rows(row):
    high = row.astype(jnp.bfloat16).astype(jnp.float32)
    index = lax.broadcasted_iota(jnp.int32, (16, row.shape[1]), 0)
    return jnp.where(index == 0, high, jnp.where(index == 1, row - high, 0.0)).astype(jnp.bfloat16)


def whole_max(array):
    return jnp.max(jnp.max(array, axis=0, keepdims=True), axis=1, keepdims=True)


def halves():
    me, devices, columns = place()
    half = devices // 2
    side = lax.div(me, half)
    return side, me - side * half, half, columns


def wrapped(value, size):
    return value - jnp.where(value >= size, size, 0)


def spot(other, step):
    side, mine, half, columns = halves()
    near = wrapped(mine + step, half)
    base = (1 - side) * half if other else side * half
    return near, base + near


def start_copy(source, target, sems, index, where, arrival=None):
    pltpu.make_async_remote_copy(
        src_ref=source,
        dst_ref=target,
        send_sem=sems[0].at[index],
        recv_sem=sems[1].at[index if arrival is None else arrival],
        device_id=where,
        device_id_type=LOGICAL,
    ).start()


def wait_blocks(ref, count, sem):
    blocks = ref if count is None else ref.at[pl.ds(0, count)]
    pltpu.make_async_copy(blocks, blocks, sem).wait()


def plan_kernel(
    support_in, source_in, target_in, mass_in, target_mass_in, coarse_in,
    f_ref, g_ref, flag_ref,
    support_ref, names_ref, source_ref, target_ref, mass_ref, target_mass_ref, coarse_ref, input_sem,
    codes, codes_scalar, asked_near, asked_far, asked_scalar, slots_ref,
    near, mate_near, tile_out, tiles,
    beta_out, mate_beta_out, betas, mate_betas, beta_next_out, beta_next,
    columns, parts, columns_next, parts_next,
    asked, requests, owners_of,
    left, weight, sums, level_f, peaks, lifted, hot, rows,
    local_sem, send_sem, recv_sem, near_sem, mate_sem, *more,
):
    _, devices, _ = place()
    side, mine, half, _ = halves()
    inputs = (support_in, support_in, source_in, target_in, mass_in, target_mass_in, coarse_in)
    landings = (support_ref, names_ref, source_ref, target_ref, mass_ref, target_mass_ref, coarse_ref)
    clusters, features, points = source_ref.shape
    entries = support_ref.shape[1]
    slots = devices * CAP
    sems = (send_sem, recv_sem)
    mates, mate_outs, mate_tiles, stores = more[:CHUNKS], more[CHUNKS : 2 * CHUNKS], more[2 * CHUNKS : 3 * CHUNKS], more[3 * CHUNKS :]
    roomy = len(stores) == 3
    barrier = pltpu.get_barrier_semaphore()

    def each_peer(use, between=None):
        for other in range(2):
            if other and between is not None:
                between()

            def one(step, carry):
                use(other, *spot(other, step))
                return carry

            lax.fori_loop(1 - other, half, one, 0, unroll=8 if other else 5)

    each_peer(
        lambda other, near, where: pl.semaphore_signal(barrier, inc=1, device_id=where, device_id_type=LOGICAL)
    )
    loads = [
        pltpu.make_async_copy(origin, landing, input_sem.at[index])
        for index, (origin, landing) in enumerate(zip(inputs, landings))
    ]
    for load in loads:
        load.start()
    for load in loads:
        load.wait()

    block = lax.broadcasted_iota(jnp.int32, (devices, entries), 0)
    far = jnp.where(block >= half, 1, 0)
    owner_of_block = jnp.where(far == 1, 1 - side, side) * half + block - far * half
    first = jnp.full((devices, entries), clusters, jnp.int32)
    second = jnp.full((devices, entries), -1, jnp.int32)
    for cluster in range(clusters):
        name = names_ref[cluster : cluster + 1, :]
        within = name - owner_of_block * clusters
        named = (within >= 0) & (within < clusters)
        first = jnp.minimum(first, jnp.where(named, within, clusters))
        second = jnp.maximum(second, jnp.where(named, within, -1))
    first = jnp.min(first, axis=1, keepdims=True)
    second = jnp.max(second, axis=1, keepdims=True)
    own = jnp.broadcast_to(first * clusters + second, (devices, points))
    swapped = jnp.concatenate([own[half:], own[:half]], axis=0)
    lane = lax.broadcasted_iota(jnp.int32, (devices, points), 1)
    codes[...] = jnp.where(lane < points // 2, own, swapped).reshape(devices, 1, points)
    slot_block = lax.broadcasted_iota(jnp.int32, (slots, entries), 0)
    pair_first = jnp.broadcast_to(first.reshape(devices, 1, 1), (devices, CAP, entries)).reshape(slots, entries)
    pair_second = jnp.broadcast_to(second.reshape(devices, 1, 1), (devices, CAP, entries)).reshape(slots, entries)
    slot_device = lax.div(slot_block, CAP)
    slot_far = jnp.where(slot_device >= half, 1, 0)
    slot_owner = jnp.where(slot_far == 1, 1 - side, side) * half + slot_device - slot_far * half
    slot_name = slot_owner * clusters + jnp.where(lax.rem(slot_block, CAP) == 0, pair_first, pair_second)
    near[...] = 2.0 * coarse_ref[...] + target_mass_ref[...]
    pl.semaphore_wait(barrier, devices - 1)

    def ask(other, near_index, where):
        start_copy(
            codes.at[other * half + near_index], (asked_far if other else asked_near).at[mine], sems, other, where
        )

    chunk = features // CHUNKS

    def relay():
        where = spot(1, 0)[1]
        start_copy(near, mate_near, sems, 3, where)
        for index in range(CHUNKS):
            start_copy(target_ref.at[:, pl.ds(index * chunk, chunk)], mates[index], sems, RELAY + index, where)

    each_peer(ask, relay)
    local = pltpu.make_async_copy(codes, codes_scalar, local_sem.at[0])
    local.start()

    def prepare_source(cluster, carry):
        wide = source_ref[cluster].astype(jnp.float32)
        square = jnp.sum(wide * wide, axis=0, keepdims=True)
        stacked = jnp.concatenate([4.0 * wide, bias_rows(LIFT - 2.0 * square, False)], axis=0)
        left[pl.ds(cluster * points, points), :] = stacked.T.astype(jnp.bfloat16)
        return carry

    lax.fori_loop(0, clusters, prepare_source, 0, unroll=2)
    local.wait()
    asked_near[mine] = codes[mine]
    wait_blocks(asked_near, half - 1, recv_sem.at[0])
    scalars = pltpu.make_async_copy(asked_near, asked_scalar, local_sem.at[1])
    scalars.start()
    scalars.wait()

    def picks(index, lane):
        code = asked_scalar[index, 0, lane]
        chosen = lax.div(code, clusters)
        return enumerate((chosen, code - chosen * clusters))

    def member(which, offset):
        quarter = half // 2
        group = lax.div(mine, quarter)
        base = (1 - group) * quarter if which else group * quarter
        return base + wrapped(mine - group * quarter + offset, quarter)

    def serve(origin, outgoing, incoming, lane, index, arrival, shift):
        for entry, pick in picks(mine, lane):
            outgoing[mine, entry] = origin[pick]
        pltpu.make_async_copy(outgoing.at[mine], incoming.at[mine], arrival.at[shift + mine]).start()
        for which in (0, 1):

            def one(step, carry):
                near_index = member(which, step)
                for entry, pick in picks(near_index, lane):
                    outgoing[near_index, entry] = origin[pick]
                start_copy(
                    outgoing.at[near_index],
                    incoming.at[mine],
                    (send_sem, arrival),
                    index,
                    side * half + near_index,
                    shift + mine,
                )
                return carry

            lax.fori_loop(1 - which, half // 2, one, 0, unroll=4 if which else half // 2 - 1)

    def serve_row(origin, outgoing, incoming, lane, index):
        def one(step, carry):
            near_index, where = spot(0, step)
            for entry, pick in picks(near_index, lane):
                outgoing[near_index, pl.ds(entry, 1), :] = origin[pl.ds(pick, 1), :]
            start_copy(outgoing.at[near_index], incoming.at[mine], sems, index, where)
            return carry

        lax.fori_loop(1, half, one, 0, unroll=5)
        for entry, pick in picks(mine, lane):
            incoming[mine, pl.ds(entry, 1), :] = origin[pl.ds(pick, 1), :]

    wait_blocks(mate_near, None, recv_sem.at[3])
    serve_row(near, beta_out, betas, 0, 5)
    serve_row(mate_near, mate_beta_out, mate_betas, points // 2, 7)
    serve(target_ref, tile_out, tiles, 0, 4, near_sem, 0)

    def place_slots(cluster, carry):
        for entry in range(entries):
            name = support_ref[cluster, entry]
            owner = lax.div(name, clusters)
            owner_side = lax.div(owner, half)
            to = lax.rem(owner_side + side, 2) * half + owner - owner_side * half
            late = name - owner * clusters > lax.div(codes_scalar[to, 0, 0], clusters)
            slots_ref[cluster, entry] = to * CAP + late.astype(jnp.int32)
        return carry

    lax.fori_loop(0, clusters, place_slots, 0)
    for cluster in range(clusters):
        hot[:, cluster * entries : (cluster + 1) * entries] = jnp.where(
            names_ref[cluster : cluster + 1, :] == slot_name, 1.0, 0.0
        )
    def set_weights(values):
        top = whole_max(values)
        weight[...] = jnp.exp(values - top)
        return top

    def joined(sources, owner, entry):
        return jnp.concatenate([source[owner, entry] for source in sources], axis=0)

    def augmented(tile):
        wide = tile.astype(jnp.float32)
        square = jnp.sum(wide * wide, axis=0, keepdims=True)
        extra = bias_rows(LIFT - 2.0 * square, True).astype(jnp.bfloat16)
        return jnp.concatenate([tile, extra], axis=0)

    def arrivals(sources, arrival, use, begin, end):
        for which in range(2):

            def one(step, carry):
                owners = []
                for lane in range(TOGETHER):
                    owner = member(which, half // 2 - (step * TOGETHER + lane))
                    for index, source in enumerate(sources):
                        wait_blocks(source.at[owner], None, arrival.at[index * half + owner])
                    owners.append(owner)
                use(owners)
                return carry

            steps = half // 2 // TOGETHER
            lax.fori_loop(
                max(begin - which * steps, 0), max(min(end - which * steps, steps), 0), one, 0
            )

    def serve_mates(index):
        wait_blocks(mates[index], None, recv_sem.at[RELAY + index])
        serve(
            mates[index], mate_outs[index], mate_tiles[index], points // 2, PASS + index, mate_sem, index * half
        )

    def set_asked():
        wait_blocks(asked_far, half, recv_sem.at[1])
        asked_own = jnp.concatenate([asked_near[...], asked_far[...]], axis=0)[:, :, 0:1]
        asked_code = jnp.broadcast_to(asked_own, (devices, CAP, points))
        asked_first = lax.div(asked_code, clusters)
        picked = jnp.where(
            lax.broadcasted_iota(jnp.int32, (devices, CAP, points), 1) == 0,
            asked_first,
            asked_code - asked_first * clusters,
        ).reshape(slots, points)
        asked[...] = picked
        matrix = jnp.where(picked == lax.broadcasted_iota(jnp.int32, (slots, points), 1), 1.0, 0.0)
        requests[...] = matrix.astype(jnp.bfloat16)
        owners_of[...] = matrix.T[:clusters].astype(jnp.bfloat16)

    def spread(values, count):
        padded = jnp.concatenate([values, jnp.zeros((points - clusters, points), jnp.float32)], axis=0)
        total = jnp.zeros((slots, points), jnp.float32)
        for _ in range(count):
            piece = padded.astype(jnp.bfloat16)
            total = total + jnp.dot(requests[...], piece, preferred_element_type=jnp.float32)
            padded = padded - piece.astype(jnp.float32)
        return total

    def owned_levels(parts_ref):
        values = parts_ref[...].reshape(slots, points)
        names = asked[...]
        peak = jnp.concatenate(
            [
                jnp.max(jnp.where(names == cluster, values, lowest), axis=0, keepdims=True)
                for cluster in range(clusters)
            ],
            axis=0,
        )
        peak = peak.astype(jnp.bfloat16).astype(jnp.float32)
        shares = jnp.exp(values - spread(peak, 1))
        total = jnp.zeros((clusters, points), jnp.float32)
        for _ in range(2):
            piece = shares.astype(jnp.bfloat16)
            total = total + jnp.dot(owners_of[...], piece, preferred_element_type=jnp.float32)
            shares = shares - piece.astype(jnp.float32)
        return peak + jnp.log(total)

    groups = half // TOGETHER
    early = groups * EARLY // 8
    for index in range(CHUNKS - 1):
        serve_mates(index)
    wait_blocks(betas, half - 1, recv_sem.at[5])
    wait_blocks(mate_betas, half - 1, recv_sem.at[7])
    start = jnp.concatenate([betas[...], mate_betas[...]], axis=0).reshape(slots, points)
    start_top = set_weights(start)

    if roomy:
        store, gathered, total_store = stores
        span = clusters // 2
        for cluster in range(clusters):
            count = jnp.sum(hot[:, cluster * entries : (cluster + 1) * entries], axis=1, keepdims=True)
            gathered[cluster] = weight[...] * count
        total_store[...] = jnp.zeros(total_store.shape, jnp.float32)

        def use_tile(sources, offset):
            def use(owners):
                picked = [(owner, entry) for owner in owners for entry in range(CAP)]
                rhs = jnp.concatenate([augmented(joined(sources, owner, entry)) for owner, entry in picked], axis=1)
                for part in range(2):
                    first_row = part * span * points
                    values = jnp.exp(
                        jnp.dot(
                            left[first_row : first_row + span * points, :], rhs, preferred_element_type=jnp.float32
                        )
                    )
                    for lane, (owner, entry) in enumerate(picked):
                        slot = (offset + owner) * CAP + entry
                        store[slot, first_row : first_row + span * points, :] = values[
                            :, lane * points : (lane + 1) * points
                        ].astype(jnp.bfloat16)
                    for index in range(span):
                        cluster = part * span + index
                        added = 0.0
                        for lane, (owner, entry) in enumerate(picked):
                            block = values[index * points : (index + 1) * points, lane * points : (lane + 1) * points]
                            slot = (offset + owner) * CAP + entry
                            added = added + block * gathered[cluster, pl.ds(slot, 1), :]
                        total_store[cluster] += added

            return use

    else:
        right, store_even, store_odd = stores[:3]

        def use_tile(sources, offset):
            def use(owners):
                for owner in owners:
                    for entry in range(CAP):
                        right[(offset + owner) * CAP + entry] = augmented(joined(sources, owner, entry))

            return use

    arrivals([tiles], near_sem, use_tile([tiles], 0), 0, early)
    serve_mates(CHUNKS - 1)
    arrivals([tiles], near_sem, use_tile([tiles], 0), early, groups)
    set_asked()
    arrivals(mate_tiles, mate_sem, use_tile(mate_tiles, half), 0, groups)
    def close(cluster, total, top):
        row = jnp.sum(total.T, axis=0, keepdims=True)
        level = jnp.log(row) + (top - 2.0 * LIFT)
        alpha = mass_ref[pl.ds(cluster, 1), :] - level
        peak = jnp.max(alpha, axis=1, keepdims=True)
        sums[pl.ds(cluster, 1), :] = row
        level_f[pl.ds(cluster, 1), :] = level
        peaks[pl.ds(cluster, 1), :] = jnp.broadcast_to(peak, (1, points))
        lifted[cluster] = split_rows(jnp.exp(alpha - peak))

    def blocks(cluster, held, pair):
        if roomy:
            return [
                held[0][slots_ref[cluster, 2 * pair + lane], pl.ds(cluster * points, points), :] for lane in range(2)
            ]
        pairs = held[0][held[1], :, pl.ds(pair * 2 * points, 2 * points)]
        return [pairs[:, lane * points : (lane + 1) * points] for lane in range(2)]

    def build(cluster, held, pair, total):
        chosen = [slots_ref[cluster, 2 * pair + lane] for lane in range(2)]
        rhs = jnp.concatenate([right[slot] for slot in chosen], axis=1)
        values = jnp.exp(
            jnp.dot(left[pl.ds(cluster * points, points), :], rhs, preferred_element_type=jnp.float32)
        )
        held[0][held[1], :, pl.ds(pair * 2 * points, 2 * points)] = values.astype(jnp.bfloat16)
        for lane, slot in enumerate(chosen):
            total = total + values[:, lane * points : (lane + 1) * points] * weight[pl.ds(slot, 1), :]
        return total

    def forward(cluster, held, pair, total):
        for lane, values in enumerate(blocks(cluster, held, pair)):
            slot = slots_ref[cluster, 2 * pair + lane]
            total = total + values.astype(jnp.float32) * weight[pl.ds(slot, 1), :]
        return total

    def backward(cluster, held, pair):
        products = jnp.dot(
            lifted[cluster],
            jnp.concatenate(blocks(cluster, held, pair), axis=1),
            preferred_element_type=jnp.float32,
        )
        row = products[0:1] + products[1:2]
        for lane in range(2):
            rows[pl.ds(cluster * entries + 2 * pair + lane, 1), :] = row[:, lane * points : (lane + 1) * points]

    def even(index):
        return (store,) if roomy else (store_even, index)

    def odd(index):
        return (store,) if roomy else (store_odd, index)

    def sweep(make, top):
        def mixed(cluster, held, before, held_before):
            total = None if cluster is None else total_store[cluster] if make is None else jnp.zeros((points, points), jnp.float32)
            done = []
            pairs = entries // 2
            for part in range(PARTS):
                for pair in range(part * pairs // PARTS, (part + 1) * pairs // PARTS):
                    if before is not None:
                        backward(before, held_before, pair)
                    if make is not None and cluster is not None:
                        total = make(cluster, held, pair, total)
            if cluster is not None:
                close(cluster, jnp.concatenate(done, axis=0) if done else total, top)

        def both(index, carry):
            mixed(2 * index + 1, odd(index), 2 * index, even(index))
            mixed(2 * index + 2, even(index + 1), 2 * index + 1, odd(index))
            return carry

        last = clusters // 2 - 1
        mixed(0, even(0), None, None)
        lax.fori_loop(0, last, both, 0)
        mixed(clusters - 1, odd(last), clusters - 2, even(last))
        mixed(None, None, clusters - 1, odd(last))
        return finish()

    def finish():
        peak = whole_max(peaks[...])
        scale = jnp.exp(peaks[...] - peak)
        total = jnp.zeros((slots, points), jnp.float32)
        values = jnp.concatenate(
            [
                rows[pl.ds(cluster * entries, entries), :] * scale[cluster : cluster + 1, :]
                for cluster in range(clusters)
            ],
            axis=0,
        )
        choice = hot[...].astype(jnp.bfloat16)
        for _ in range(2):
            piece = values.astype(jnp.bfloat16)
            total = total + jnp.dot(choice, piece, preferred_element_type=jnp.float32)
            values = values - piece.astype(jnp.float32)
        low = jnp.maximum(
            whole_max(jnp.where(sums[...] >= FLOOR, 0.0, 1.0)), whole_max(jnp.where(total >= FLOOR, 0.0, 1.0))
        )
        column = jnp.log(total) + (peak - 2.0 * LIFT)
        return jnp.where(low > 0.0, ALARM, column).reshape(devices, CAP, points)

    def return_columns(source, target, index):
        each_peer(
            lambda other, near_index, where: start_copy(
                source.at[other * half + near_index], target.at[other * half + mine], sems, index, where
            )
        )
        target[mine] = source[mine]
        wait_blocks(target, devices - 1, recv_sem.at[index])

    columns[...] = sweep(None if roomy else build, start_top)
    return_columns(columns, parts, 8)
    beta_next_out[...] = spread(target_mass_ref[...] - owned_levels(parts), 3).reshape(devices, CAP, points)
    return_columns(beta_next_out, beta_next, 9)
    columns_next[...] = sweep(forward, set_weights(beta_next[...].reshape(slots, points)))
    f_ref[...] = level_f[...]
    return_columns(columns_next, parts_next, 10)
    g_ref[...] = owned_levels(parts_next)
    alarm = jnp.maximum(parts[...].reshape(slots, points), parts_next[...].reshape(slots, points))
    flag_ref[0, 0] = jnp.max(jnp.where(alarm < 1e30, 0.0, 1.0)).astype(jnp.int32)
    wait_blocks(codes, half - 1, send_sem.at[0])
    wait_blocks(codes, half, send_sem.at[1])
    for index in range(CHUNKS):
        wait_blocks(mates[index], None, send_sem.at[RELAY + index])
        wait_blocks(mate_outs[index], half - 1, send_sem.at[PASS + index])
    wait_blocks(near, None, send_sem.at[3])
    wait_blocks(tile_out, half - 1, send_sem.at[4])
    wait_blocks(beta_out, half - 1, send_sem.at[5])
    wait_blocks(mate_beta_out, half - 1, send_sem.at[7])
    wait_blocks(columns, devices - 1, send_sem.at[8])
    wait_blocks(beta_next_out, devices - 1, send_sem.at[9])
    wait_blocks(columns_next, devices - 1, send_sem.at[10])


def plan_call(support, source, target, mass, target_mass, coarse):
    devices = lax.axis_size(AXES)
    clusters, features, points = source.shape
    entries = support.shape[1]
    slots = devices * CAP
    half = devices // 2
    depth = features + EXTRA
    vmem = pl.BlockSpec(memory_space=pltpu.VMEM)
    level = jax.ShapeDtypeStruct((clusters, points), jnp.float32)
    levels = pltpu.VMEM((clusters, points), jnp.float32)
    row_block = pltpu.VMEM((devices, CAP, points), jnp.float32)
    half_row = pltpu.VMEM((half, CAP, points), jnp.float32)
    half_tile = pltpu.VMEM((half, CAP, features, points), jnp.bfloat16)
    whole_tile = pltpu.VMEM((clusters, features, points), jnp.bfloat16)
    half_code = pltpu.VMEM((half, 1, points), jnp.int32)
    roomy = slots * clusters * points * points <= ROOM
    if roomy:
        stores = [
            pltpu.VMEM((slots, clusters * points, points), jnp.bfloat16),
            pltpu.VMEM((clusters, slots, points), jnp.float32),
            pltpu.VMEM((clusters, points, points), jnp.float32),
        ]
    else:
        kernel_block = pltpu.VMEM((clusters // 2, points, entries * points), jnp.bfloat16)
        stores = [pltpu.VMEM((slots, depth, points), jnp.bfloat16), kernel_block, kernel_block, pltpu.SMEM((1,), jnp.int32)]
    sems = pltpu.SemaphoreType.DMA((PASS + CHUNKS,))
    return pl.pallas_call(
        plan_kernel,
        out_shape=(level, level, jax.ShapeDtypeStruct((1, 1), jnp.int32)),
        in_specs=[pl.BlockSpec(memory_space=pltpu.HBM)] * 6,
        out_specs=(vmem, vmem, pl.BlockSpec(memory_space=pltpu.SMEM)),
        scratch_shapes=[
            pltpu.SMEM((clusters, entries), jnp.int32),
            pltpu.VMEM((clusters, entries), jnp.int32),
            whole_tile,
            whole_tile,
            levels, levels, levels,
            pltpu.SemaphoreType.DMA((7,)),
            pltpu.VMEM((devices, 1, points), jnp.int32),
            pltpu.SMEM((devices, 1, points), jnp.int32),
            half_code,
            half_code,
            pltpu.SMEM((half, 1, points), jnp.int32),
            pltpu.SMEM((clusters, entries), jnp.int32),
            levels,
            levels,
            half_tile, half_tile,
            half_row, half_row, half_row, half_row,
            row_block, row_block, row_block, row_block, row_block, row_block,
            pltpu.VMEM((slots, points), jnp.int32),
            pltpu.VMEM((slots, points), jnp.bfloat16),
            pltpu.VMEM((clusters, slots), jnp.bfloat16),
            pltpu.VMEM((clusters * points, depth), jnp.bfloat16),
            pltpu.VMEM((slots, points), jnp.float32),
            levels, levels, levels,
            pltpu.VMEM((clusters, 16, points), jnp.bfloat16),
            pltpu.VMEM((slots, clusters * entries), jnp.float32),
            pltpu.VMEM((clusters * entries, points), jnp.float32),
            pltpu.SemaphoreType.DMA((2,)), sems, sems,
            pltpu.SemaphoreType.DMA((half,)), pltpu.SemaphoreType.DMA((CHUNKS * half,)),
        ]
        + [pltpu.VMEM((clusters, features // CHUNKS, points), jnp.bfloat16)] * CHUNKS
        + [pltpu.VMEM((half, CAP, features // CHUNKS, points), jnp.bfloat16)] * (2 * CHUNKS)
        + stores,
        compiler_params=pltpu.CompilerParams(
            collective_id=8, has_side_effects=True, vmem_limit_bytes=60 * 1024 * 1024
        ),
        name="plan",
    )(support, source, target, mass, target_mass, coarse)


def careful(source_points, target_points, source_mass, target_mass, support, coarse_potential):
    devices = lax.axis_size(AXES)
    local_count, features, points = source_points.shape
    owner = support // local_count
    within = support % local_count
    flat_owner, flat_within = owner.reshape(-1), within.reshape(-1)
    named = flat_owner[None, :] == jnp.arange(devices, dtype=jnp.int32)[:, None]
    first = jnp.min(jnp.where(named, flat_within[None, :], local_count), axis=1)
    second = jnp.max(jnp.where(named, flat_within[None, :], -1), axis=1)
    request = jnp.stack([first, second], axis=1).astype(jnp.int32)
    shape = (devices, CAP, points)
    (asked,) = exchange([jnp.broadcast_to(request[:, :, None], shape)], 0)
    first_of = jnp.sum(jnp.where(named, first[:, None], 0), axis=0).reshape(owner.shape)
    slot_list = (owner * CAP + (within > first_of).astype(jnp.int32)).astype(jnp.int32)

    target_sq = squares(target_points)
    source_sq = squares(source_points)
    u = 2.0 * (coarse_potential - target_sq) + target_mass
    matches = asked[:, :, None, :] == jnp.arange(local_count, dtype=jnp.int32)[:, None]
    sending = jnp.sum(jnp.where(matches, u, 0.0), axis=2)
    tiles, received = exchange([target_points[asked[:, :, 0]], sending], 1)
    tiles = tiles.reshape(devices * CAP, features, points)
    row_shape = jax.ShapeDtypeStruct(shape, jnp.float32)
    level_shape = jax.ShapeDtypeStruct(target_mass.shape, jnp.float32)
    buffer = pltpu.VMEM(shape, jnp.float32)
    for sweep in range(ITERS):
        level, column = sweep_call(
            slot_list, source_points, source_mass, tiles, received.reshape(devices * CAP, points)
        )
        column = column.reshape(shape)
        if sweep < ITERS - 1:
            received = owner_call(
                turn_kernel, row_shape, [buffer, buffer], 2 + sweep, column, asked, target_mass
            )
    column_level = owner_call(finish_kernel, level_shape, [buffer], 1 + ITERS, column, asked)
    return level - 2.0 * source_sq, column_level - 2.0 * target_sq


def body(source_points, target_points, source_mass, target_mass, support, coarse_potential):
    f, g, flag = plan_call(
        support, source_points, target_points, source_mass, target_mass, coarse_potential
    )

    def again():
        return careful(
            source_points, target_points, source_mass, target_mass, support, coarse_potential
        )

    f, g = lax.cond(flag[0, 0] > 0, again, lambda: (f, g))
    return -0.5 * f, -0.5 * g


def solution(mesh):
    placed = (
        P(AXES, None, None),
        P(AXES, None, None),
        P(AXES, None),
        P(AXES, None),
        P(AXES, None),
        P(AXES, None),
    )
    return jax.shard_map(
        body,
        mesh=mesh,
        in_specs=placed,
        out_specs=(P(AXES, None), P(AXES, None)),
        check_vma=False,
    )
```
